512 devices in a mesh: row: 32 (over x, y_lo, core), col: 16 (over y_hi, z).
Axes of the slice: x: 4, y: 8 (y_hi: 2, y_lo: 4; y = y_hi * 4 + y_lo), z: 8, core: 2. Of those that a mesh axis runs over, the one named last changes fastest.
Arguments:
- object_slices: float32 [2, 2, 4096, 2048], P(None, None, 'row', 'col'), may hold values from -5 to 5
- probe: float32 [2, 256, 256], replicated, may hold values from -6 to 6
- offsets: int32 [32, 16, 1, 2], P('row', 'col'), may hold values from 0 to 127
- residuals: float32 [32, 16, 1, 2, 256, 256], P('row', 'col'), may hold values from -6 to 6
Outputs:
- new_object: float32 [2, 2, 4096, 2048], P(None, None, 'row', 'col')
The draws below stay inside these ranges and needn't reach their ends.
All inputs are finite; a program needn't handle non-finite values.
Results may differ from the reference program's by a relative error of at most 0.0003.
Values sent between devices are 32-bit elements; how exact they have to be, the bound alone decides.
A program may use at most 64 MiB of HBM per device.

```python
import jax
import jax.numpy as jnp
from jax import lax

WIN = 256
NS = 2
POS_DEV = 1
TILE = 128
N_ROW = 32
N_COL = 16


def with_ends(result, own_key, least, largest):
    longest = result.shape.index(max(result.shape))
    spots = []
    for shift in (0, 1):
        where = [jax.random.randint(jax.random.fold_in(own_key, axis), (), 0, length) for axis, length in enumerate(result.shape)]
        where[longest] = (where[longest] + shift) % result.shape[longest]
        spots.append(tuple(where))
    return result.at[spots[0]].set(least).at[spots[1]].set(largest)


def levels(key, extent, shards, least, largest):
    level, own = 1.0, jax.random.fold_in(key, 6)
    for axis_at, blocks in shards:
        draws = jnp.exp(jax.random.uniform(jax.random.fold_in(own, axis_at), (blocks,), jnp.float32, least / len(shards), largest / len(shards)))
        level = level * jnp.repeat(draws, extent[axis_at] // blocks).reshape([-1 if axis == axis_at else 1 for axis in range(len(extent))])
    return level


def scatter_about(key, extent, deviation, bound, cuts=(), kind=jnp.bfloat16):
    gain = levels(key, extent, cuts, -0.22, 0.18) if cuts else 1.0
    drawn = jax.random.normal(key, extent, jnp.float32) * deviation * gain
    return jnp.minimum(jnp.maximum(drawn, -bound), bound).astype(kind)


def setup_inputs(seed: int = 0) -> dict:
    arg_keys = jax.random.split(jax.random.key(seed), 5)
    object_slices = scatter_about(arg_keys[0], (NS, 2, TILE * N_ROW, TILE * N_COL), 0.7, 5.0, ((2, 32), (3, 16)), jnp.float32)
    probe = scatter_about(arg_keys[1], (2, WIN, WIN), 1.0, 6.0, (), jnp.float32)
    offsets = with_ends(jax.random.randint(arg_keys[2], (N_ROW, N_COL, POS_DEV, 2), 0, TILE), jax.random.fold_in(arg_keys[2], 1), 0, TILE - 1).astype(jnp.int32)
    residuals = scatter_about(arg_keys[3], (N_ROW, N_COL, POS_DEV, 2, WIN, WIN), 1.0, 6.0, ((0, 32), (1, 16)), jnp.float32)
    return dict(object_slices=object_slices, probe=probe, offsets=offsets, residuals=residuals)


FRESNEL = 40.0
STEP_SIZE = 0.5
REGULAR = 1.0


def kernel_phase():
    index = jnp.arange(WIN, dtype=jnp.int32)
    freq = jnp.where(index < WIN // 2, index, index - WIN).astype(jnp.float32) / WIN
    phase = FRESNEL * jnp.pi * freq * freq
    return phase[:, None] + phase[None, :]


def propagate(wave, phase, direction):
    spectrum = jnp.fft.fft2(wave, norm="ortho")
    return jnp.fft.ifft2(spectrum * jnp.exp(-1j * direction * phase), norm="ortho")


def one_position(window, probe_wave, resid, phase):
    waves = [probe_wave]
    wave = probe_wave
    for layer in range(NS - 1):
        wave = propagate(wave * window[layer], phase, 1.0)
        waves.append(wave)
    back = jnp.fft.ifft2(resid, norm="ortho")
    parts = [None] * NS
    for layer in reversed(range(NS)):
        current = waves[layer]
        term = jnp.conj(current) * back
        light = jnp.real(current) * jnp.real(current) + jnp.imag(current) * jnp.imag(current)
        parts[layer] = jnp.stack([jnp.real(term), jnp.imag(term), light])
        if layer > 0:
            back = propagate(jnp.conj(window[layer]) * back, phase, -1.0)
    return jnp.stack(parts)


def reference(object_slices, probe, offsets, residuals):
    height = TILE * N_ROW
    breadth = TILE * N_COL
    whole = object_slices[:, 0] + 1j * object_slices[:, 1]
    padded = jnp.concatenate([whole, whole[:, :2 * TILE]], axis=1)
    padded = jnp.concatenate([padded, padded[:, :, :2 * TILE]], axis=2)
    probe_wave = probe[0] + 1j * probe[1]
    phase = kernel_phase()
    buffer = jnp.zeros((NS, 3, height + 2 * TILE, breadth + 2 * TILE), jnp.float32)

    def visit(buffer, tile_id):
        tile_row = tile_id // N_COL
        tile_col = tile_id % N_COL
        zero = jnp.zeros((), jnp.int32)
        for slot in range(POS_DEV):
            top = (tile_row * TILE + offsets[tile_row, tile_col, slot, 0]).astype(jnp.int32)
            left = (tile_col * TILE + offsets[tile_row, tile_col, slot, 1]).astype(jnp.int32)
            window = lax.dynamic_slice(padded, (zero, top, left), (NS, WIN, WIN))
            pair = residuals[tile_row, tile_col, slot]
            resid = pair[0] + 1j * pair[1]
            contrib = one_position(window, probe_wave, resid, phase).astype(jnp.float32)
            older = lax.dynamic_slice(buffer, (zero, zero, top, left), (NS, 3, WIN, WIN))
            buffer = lax.dynamic_update_slice(buffer, older + contrib, (zero, zero, top, left))
        return buffer, None

    tiles = jnp.arange(N_ROW * N_COL, dtype=jnp.int32)
    buffer, unused = lax.scan(visit, buffer, tiles)
    buffer = buffer.at[:, :, :2 * TILE].add(buffer[:, :, height:])
    buffer = buffer[:, :, :height]
    buffer = buffer.at[:, :, :, :2 * TILE].add(buffer[:, :, :, breadth:])
    buffer = buffer[:, :, :, :breadth]
    gradient = buffer[:, 0:2]
    illumination = buffer[:, 2:3]
    return object_slices - STEP_SIZE * gradient / (illumination + REGULAR)
```

```python
import math

import jax
import jax.numpy as jnp
import numpy as np
from jax import lax
from jax.experimental import pallas as pl
from jax.experimental.pallas import tpu as pltpu
from jax.sharding import PartitionSpec as P

FRESNEL = 40.0
STEP_SIZE = 0.5
REGULAR = 1.0
MESH = pl.DeviceIdType.MESH
F32 = jnp.float32
BF16 = jnp.bfloat16


def halves(mat):
    high = mat.astype(jnp.bfloat16)
    low = (mat - high.astype(np.float64)).astype(jnp.bfloat16)
    return [high, low]


def tables(width):
    index = np.arange(width)
    angle = 2.0 * math.pi / width * ((index[:, None] * index[None, :]) % width)
    inverse = np.exp(1j * angle) / math.sqrt(width)
    freq = np.where(index < width // 2, index, index - width) / width
    kern = np.exp(-1j * FRESNEL * math.pi * freq * freq)
    prop = (inverse * kern[None, :]) @ np.conj(inverse)
    pack = lambda mat: np.stack(halves(mat.real) + halves(mat.imag))
    return pack(inverse), pack(prop)


def split(value):
    high = value.astype(BF16)
    return high, (value - high.astype(F32)).astype(BF16)


def dot(left, right):
    return jnp.dot(left, right, preferred_element_type=F32)


def names():
    found = {}
    for kind, count in (("z1", 1), ("z2", 1), ("a", 3), ("b", 3), ("f", 3), ("q1", 3), ("q2", 3), ("q3", 3), ("c2", 1), ("c1", 1)):
        for layer in range(2):
            for band in range(count):
                found[kind, layer, band] = len(found)
    return found


SLOTS = names()


def kernel(
    n_row, n_col, offs, obj, probe, resid, ftab, atab, out,
    reg, work, four_r, four_l, prop_r, prop_l, half, psi0, back1, terms, rx_a, rx_b, rx_c, rx_d, tx, ssem, rsem,
):
    tile = obj.shape[2]
    width = 2 * tile
    row = lax.axis_index("row")
    col = lax.axis_index("col")
    odd = lax.rem(row, 2) == 1
    even = lax.rem(row, 2) == 0
    at = lambda dr, dc: (lax.rem(row + dr + n_row, n_row), lax.rem(col + dc + n_col, n_col))

    barrier = pltpu.get_barrier_semaphore()
    greet = lambda who: pl.semaphore_signal(barrier, inc=1, device_id=who, device_id_type=MESH)
    for who in (at(0, -1), at(0, 1), at(-1, 0), at(1, 0)):
        greet(who)

    @pl.when(odd)
    def _():
        greet(at(-2, 0))
        greet(at(2, 0))
        pl.semaphore_wait(barrier, 6)

    @pl.when(even)
    def _():
        pl.semaphore_wait(barrier, 4)

    def copy(kind, layer, band, source, target, who):
        slot = SLOTS[kind, layer, band]
        return pltpu.make_async_remote_copy(
            src_ref=source, dst_ref=target, send_sem=ssem.at[slot], recv_sem=rsem.at[slot], device_id=who, device_id_type=MESH
        )

    own = lambda s, j: obj.at[s] if j == 0 else reg.at[s, 0, j]
    z1 = lambda s: copy("z1", s, 0, obj.at[s], reg.at[s, 0, 1], at(0, -1))
    z2 = lambda s: copy("z2", s, 0, reg.at[s, 0, 1], reg.at[s, 0, 2], at(0, -1))
    step_a = lambda s, j: copy("a", s, j, own(s, j), reg.at[s, 1, j], at(-1, 0))
    step_b = lambda s, j: copy("b", s, j, own(s, j), reg.at[s, 2, j], at(-2, 0))
    step_f = lambda s, j: copy("f", s, j, reg.at[s, 1, j], reg.at[s, 2, j], at(-1, 0))
    q1 = lambda s, j: copy("q1", s, j, terms.at[s, 1, j], rx_a.at[s, j], at(1, 0))
    q1s = lambda s, j: copy("q1", s, j, tx.at[s, j], rx_a.at[s, j], at(1, 0))
    q2 = lambda s, j: copy("q2", s, j, terms.at[s, 2, j], rx_b.at[s, j], at(2, 0))
    q3 = lambda s, j: copy("q3", s, j, terms.at[s, 2, j], rx_c.at[s, j], at(1, 0))
    c2 = lambda s: copy("c2", s, 0, tx.at[s, 3], rx_d.at[s, 0], at(0, 1))
    c1 = lambda s: copy("c1", s, 0, tx.at[s, 4], rx_d.at[s, 1], at(0, 1))

    def strip(s, j):
        step_a(s, j).start()

        @pl.when(odd)
        def _():
            step_b(s, j).start()

    for s in range(2):
        z1(s).start()
        strip(s, 0)

    top = offs[0]
    left = offs[1]

    def mirrored(plain_re, plain_im, right, part):
        neg = -plain_im
        if right:
            part[0:width, 0:width] = plain_re
            part[0:width, width:] = plain_im
            part[width:, 0:width] = neg
            part[width:, width:] = plain_re
        else:
            part[0:width, 0:width] = plain_re
            part[0:width, width:] = neg
            part[width:, 0:width] = plain_im
            part[width:, width:] = plain_re

    for k in range(2):
        mirrored(atab[k], atab[2 + k], True, prop_r.at[k])
        mirrored(atab[k], atab[2 + k], False, prop_l.at[k])

    def one_hot(shift, axis):
        place = lax.broadcasted_iota(jnp.int32, (width, width), axis)
        other = lax.broadcasted_iota(jnp.int32, (width, width), 1 - axis)
        moved = place - shift
        moved = jnp.where(moved < 0, moved + width, moved)
        return jnp.where(moved == other, 1.0, 0.0).astype(BF16)

    rows_hot = one_hot(top, 0)
    cols_hot = one_hot(left, 1)
    for k in range(2):
        mirrored(dot(ftab[k], cols_hot).astype(BF16), dot(ftab[2 + k], cols_hot).astype(BF16), True, four_r.at[k])
        mirrored(dot(rows_hot, ftab[k]).astype(BF16), dot(rows_hot, ftab[2 + k]).astype(BF16), False, four_l.at[k])

    for k in range(2):
        total = None
        for part in split(probe[k]):
            moved = dot(dot(rows_hot, part).astype(BF16), cols_hot)
            total = moved if total is None else total + moved
        psi0[k] = total

    def put(k, rows, cols, value):
        high, low = split(value)
        base = k * width
        work[0, rows, base + cols.start : base + cols.stop] = high
        work[1, rows, base + cols.start : base + cols.stop] = low

    def sandwich(left_mat, right_mat):
        inner = dot(work[0], right_mat[0]) + (dot(work[1], right_mat[0]) + dot(work[0], right_mat[1]))
        for k in range(2):
            high, low = split(inner[:, k * width : (k + 1) * width])
            half[0, k * width : (k + 1) * width, :] = high
            half[1, k * width : (k + 1) * width, :] = low
        return dot(left_mat[0], half[0]) + (dot(left_mat[1], half[0]) + dot(left_mat[0], half[1]))

    everything = slice(0, width)
    for k in range(2):
        put(k, everything, everything, resid[k])
    both = sandwich(four_l, four_r)
    back1[0] = both[0:width]
    back1[1] = both[width:]

    rowm = lax.broadcasted_iota(jnp.int32, (tile, tile), 0) >= top
    colm = lax.broadcasted_iota(jnp.int32, (tile, tile), 1) >= left
    lo = slice(0, tile)
    hi = slice(tile, width)

    def piece(s, i, j, k):
        return obj[s, k] if i == 0 and j == 0 else reg[s, i, j, k]

    def quadrant(s, rows, cols, k):
        if rows is lo and cols is lo:
            return jnp.where(
                rowm,
                jnp.where(colm, piece(s, 0, 0, k), piece(s, 0, 2, k)),
                jnp.where(colm, piece(s, 2, 0, k), piece(s, 2, 2, k)),
            )
        if rows is lo:
            return jnp.where(rowm, piece(s, 0, 1, k), piece(s, 2, 1, k))
        if cols is lo:
            return jnp.where(colm, piece(s, 1, 0, k), piece(s, 1, 2, k))
        return piece(s, 1, 1, k)

    def scatter(s, ch, value):
        zero = jnp.zeros((tile, tile), F32)
        corner = value[lo, lo]
        upper = jnp.where(rowm, corner, zero)
        lower = jnp.where(rowm, zero, corner)
        terms[s, 0, 0, ch] = jnp.where(colm, upper, zero)
        terms[s, 0, 2, ch] = jnp.where(colm, zero, upper)
        terms[s, 2, 0, ch] = jnp.where(colm, lower, zero)
        terms[s, 2, 2, ch] = jnp.where(colm, zero, lower)
        corner = value[lo, hi]
        terms[s, 0, 1, ch] = jnp.where(rowm, corner, zero)
        terms[s, 2, 1, ch] = jnp.where(rowm, zero, corner)
        corner = value[hi, lo]
        terms[s, 1, 0, ch] = jnp.where(colm, corner, zero)
        terms[s, 1, 2, ch] = jnp.where(colm, zero, corner)
        terms[s, 1, 1, ch] = value[hi, hi]

    def arrivals(s):
        for j in range(3):
            step_a(s, j).wait_recv()

            @pl.when(odd)
            def _():
                step_f(s, j).start()

        for j in range(3):

            @pl.when(odd)
            def _():
                step_b(s, j).wait_recv()

            @pl.when(even)
            def _():
                step_f(s, j).wait_recv()

    for s in range(2):
        z1(s).wait_recv()
        z2(s).start()
        strip(s, 1)
    for s in range(2):
        z2(s).wait_recv()
        strip(s, 2)

    def send_terms(s):
        for j in (2, 1, 0):

            @pl.when(odd)
            def _():
                q2(s, j).start()

            @pl.when(even)
            def _():
                q3(s, j).start()
                q1(s, j).start()

    def send_sums(s):
        for j in (2, 1, 0):

            @pl.when(odd)
            def _():
                q3(s, j).wait_recv()
                tx[s, j] = terms[s, 1, j] + rx_c[s, j]
                q1s(s, j).start()

    def row_total(s, j):
        q1(s, j).wait_recv()

        @pl.when(odd)
        def _():
            q2(s, j).wait_recv()

        @pl.when(odd)
        def _():
            terms[s, 0, j] = terms[s, 0, j] + (rx_a[s, j] + rx_b[s, j])

        @pl.when(even)
        def _():
            terms[s, 0, j] = terms[s, 0, j] + rx_a[s, j]

        return terms[s, 0, j]

    arrivals(0)
    for rows in (lo, hi):
        for cols in (lo, hi):
            obj_re, obj_im = quadrant(0, rows, cols, 0), quadrant(0, rows, cols, 1)
            psi_re, psi_im = psi0[0, rows, cols], psi0[1, rows, cols]
            put(0, rows, cols, psi_re * obj_re - psi_im * obj_im)
            put(1, rows, cols, psi_re * obj_im + psi_im * obj_re)
    both = sandwich(prop_l, prop_r)
    wave_re, wave_im = both[0:width], both[width:]
    scatter(1, 0, wave_re * back1[0] + wave_im * back1[1])
    scatter(1, 1, wave_re * back1[1] - wave_im * back1[0])
    scatter(1, 2, wave_re * wave_re + wave_im * wave_im)
    send_terms(1)

    arrivals(1)
    for rows in (lo, hi):
        for cols in (lo, hi):
            obj_re, obj_im = quadrant(1, rows, cols, 0), quadrant(1, rows, cols, 1)
            back_re, back_im = back1[0, rows, cols], back1[1, rows, cols]
            put(0, rows, cols, obj_re * back_re + obj_im * back_im)
            put(1, rows, cols, obj_im * back_re - obj_re * back_im)
    send_sums(1)
    both = sandwich(prop_l, prop_r)
    conj_re, conj_im = both[0:width], both[width:]
    scatter(0, 0, psi0[0] * conj_re - psi0[1] * conj_im)
    scatter(0, 1, -(psi0[0] * conj_im + psi0[1] * conj_re))
    scatter(0, 2, psi0[0] * psi0[0] + psi0[1] * psi0[1])
    send_terms(0)

    tx[1, 3] = row_total(1, 2)
    c2(1).start()
    send_sums(0)
    middle = row_total(1, 1)
    c2(1).wait_recv()
    tx[1, 4] = middle + rx_d[1, 0]
    c1(1).start()
    tx[0, 3] = row_total(0, 2)
    c2(0).start()
    middle = row_total(0, 1)
    c2(0).wait_recv()
    tx[0, 4] = middle + rx_d[0, 0]
    c1(0).start()
    for s in (1, 0):
        last = row_total(s, 0)
        c1(s).wait_recv()
        total = last + rx_d[s, 1]
        scale = STEP_SIZE / (total[2] + REGULAR)
        for k in range(2):
            out[s, k] = obj[s, k] - total[k] * scale

    for s in range(2):
        for sent in (z1(s), z2(s), c2(s), c1(s)):
            sent.wait_send()
        for j in range(3):
            step_a(s, j).wait_send()
            q1(s, j).wait_send()

            @pl.when(odd)
            def _():
                step_b(s, j).wait_send()
                step_f(s, j).wait_send()
                q2(s, j).wait_send()

            @pl.when(even)
            def _():
                q3(s, j).wait_send()


def solution(mesh):
    n_row, n_col = mesh.shape["row"], mesh.shape["col"]

    def local(object_slices, probe, offsets, residuals):
        layers, parts, tile, _ = object_slices.shape
        width = probe.shape[1]
        four, prop = tables(width)
        vmem = pl.BlockSpec(memory_space=pltpu.VMEM)
        stack = pltpu.VMEM((2, 2 * width, 2 * width), BF16)
        block = (3, tile, tile)
        call = pl.pallas_call(
            lambda *refs: kernel(n_row, n_col, *refs),
            out_shape=jax.ShapeDtypeStruct(object_slices.shape, F32),
            in_specs=[pl.BlockSpec(memory_space=pltpu.SMEM)] + [vmem] * 5,
            out_specs=vmem,
            scratch_shapes=[
                pltpu.VMEM((layers, 3, 3, parts, tile, tile), F32),
                pltpu.VMEM((2, width, 2 * width), BF16),
                stack, stack, stack, stack,
                pltpu.VMEM((2, 2 * width, width), BF16),
                pltpu.VMEM((2, width, width), F32),
                pltpu.VMEM((2, width, width), F32),
                pltpu.VMEM((layers, 3, 3) + block, F32),
                pltpu.VMEM((layers, 3) + block, F32),
                pltpu.VMEM((layers, 3) + block, F32),
                pltpu.VMEM((layers, 3) + block, F32),
                pltpu.VMEM((layers, 2) + block, F32),
                pltpu.VMEM((layers, 5) + block, F32),
                pltpu.SemaphoreType.DMA((len(SLOTS),)),
                pltpu.SemaphoreType.DMA((len(SLOTS),)),
            ],
            compiler_params=pltpu.CompilerParams(collective_id=0, has_side_effects=True, vmem_limit_bytes=56 * 1024 * 1024),
            name="ptycho",
        )
        return call(offsets.reshape(2), object_slices, probe, residuals[0, 0, 0], jnp.asarray(four), jnp.asarray(prop))

    placed = (
        P(None, None, "row", "col"),
        P(),
        P("row", "col", None, None),
        P("row", "col", None, None, None, None),
    )
    return jax.shard_map(local, mesh=mesh, in_specs=placed, out_specs=P(None, None, "row", "col"), check_vma=False)
```

```python
import math

import jax
import jax.numpy as jnp
import numpy as np
from jax import lax
from jax.experimental import pallas as pl
from jax.experimental.pallas import tpu as pltpu
from jax.sharding import PartitionSpec as P

FRESNEL = 40.0
STEP_SIZE = 0.5
REGULAR = 1.0
MESH = pl.DeviceIdType.MESH
F32 = jnp.float32
BF16 = jnp.bfloat16


def halves(mat):
    high = mat.astype(jnp.bfloat16)
    low = (mat - high.astype(np.float64)).astype(jnp.bfloat16)
    return [high, low]


def tables(width):
    index = np.arange(width)
    angle = 2.0 * math.pi / width * ((index[:, None] * index[None, :]) % width)
    inverse = np.exp(1j * angle) / math.sqrt(width)
    freq = np.where(index < width // 2, index, index - width) / width
    kern = np.exp(-1j * FRESNEL * math.pi * freq * freq)
    prop = (inverse * kern[None, :]) @ np.conj(inverse)
    pack = lambda mat: np.stack(halves(mat.real) + halves(mat.imag))
    return pack(inverse), pack(prop)


def split(value):
    high = value.astype(BF16)
    return high, (value - high.astype(F32)).astype(BF16)


def dot(left, right):
    return jnp.dot(left, right, preferred_element_type=F32)


GATHER_PARTS = (
    (0, 64, ((0, 0), (1, 7))),
    (64, 128, ((0, 0), (0, 7), (1, 7))),
)
SUM_PARTS = (
    (0, 64, ((0, 7), (1, 0))),
    (64, 128, ((0, 7), (0, 0), (1, 0))),
)


def names():
    found = {}
    kinds = (("z1", 1), ("z2", 1), ("a", 3), ("b", 3), ("f", 3), ("q1", 3), ("q2", 3), ("q3", 3), ("c2", 1), ("c1", 1))
    for kind, count in kinds:
        for layer in range(2):
            for band in range(count):
                found[kind, layer, band] = len(found)
    for kind in ("z1", "z2", "c2", "c1"):
        for layer in range(2):
            for k, part in enumerate(GATHER_PARTS if kind[0] == "z" else SUM_PARTS):
                for leg in range(len(part[2]) - 1):
                    found[kind, layer, (k, leg)] = len(found)
    for band in range(4):
        found["o", 0, band] = len(found)
    return found


SLOTS = names()


def kernel(
    n_row, n_col, offs, obj, probe, resid, ftab, atab, out,
    reg, work, four_r, four_l, prop_r, prop_l, half, psi0, back1, terms, rx_a, rx_b, rx_c, rx_d, tx, relay_z, relay_c, places, row_hot, col_hot, picked, light0, ssem, rsem,
):
    tile = obj.shape[2]
    width = 2 * tile
    row = lax.axis_index("row")
    col = lax.axis_index("col")
    odd = lax.rem(row, 2) == 1
    even = lax.rem(row, 2) == 0
    at = lambda dr, dc: (lax.rem(row + dr + n_row, n_row), lax.rem(col + dc + n_col, n_col))

    depth = n_col // 2
    plane = lax.rem(col, depth)
    base = col - plane
    flipped = depth - base
    top = offs[0]
    left = offs[1]
    line = lax.broadcasted_iota(jnp.int32, places.shape[2:], 0)
    places[0, 0] = jnp.where(line == 0, top, left).astype(F32)

    barrier = pltpu.get_barrier_semaphore()
    greet = lambda who: pl.semaphore_signal(barrier, inc=1, device_id=who, device_id_type=MESH)
    for who in (at(0, -1), at(0, 1), at(0, -2), at(0, 2), at(-1, 0), at(1, 0), at(-2, 0), at(2, 0)):
        greet(who)
    count = 8
    hops = []
    for parts in (GATHER_PARTS, SUM_PARTS):
        for _, _, path in parts:
            for leg in range(len(path) - 1):
                if len(path) > 2:
                    hops.append((path[leg], path[leg + 1]))

    def place_of(node, other):
        return (row, (base if node[0] == other[0] else flipped) + other[1])

    for first, second in hops:

        @pl.when(plane == first[1])
        def _():
            greet(place_of(first, second))

        @pl.when(plane == second[1])
        def _():
            greet(place_of(second, first))

        count = count + jnp.where(plane == first[1], 1, 0) + jnp.where(plane == second[1], 1, 0)
    pl.semaphore_wait(barrier, count)

    def copy(kind, layer, band, source, target, who):
        slot = SLOTS[kind, layer, band]
        return pltpu.make_async_remote_copy(
            src_ref=source, dst_ref=target, send_sem=ssem.at[slot], recv_sem=rsem.at[slot], device_id=who, device_id_type=MESH
        )

    class Message:
        def __init__(self, kind, layer, source, target, relay, parts, step):
            self.first, self.last = parts[0][2][0][1], parts[0][2][-1][1]
            self.main = copy(kind, layer, 0, source, target, at(0, step))
            self.legs = []
            for k, (low, high, path) in enumerate(parts):
                here = source.at[:, low:high]
                for leg in range(len(path) - 1):
                    final = leg == len(path) - 2
                    there = target.at[:, low:high] if final else relay.at[leg, :, low:high]
                    who = place_of(path[leg], path[leg + 1])
                    self.legs.append((path[leg][1], path[leg + 1][1], leg == 0, final, copy(kind, layer, (k, leg), here, there, who)))
                    here = there

        def start(self):
            @pl.when(plane != self.first)
            def _():
                self.main.start()

            @pl.when(plane == self.first)
            def _():
                for _, _, opening, _, leg in self.legs:
                    if opening:
                        leg.start()

        def relay(self):
            for k, (_, sink, _, final, leg) in enumerate(self.legs):
                if not final:
                    following = self.legs[k + 1][4]

                    @pl.when(plane == sink)
                    def _():
                        leg.wait_recv()
                        following.start()

        def wait_recv(self):
            @pl.when(plane != self.last)
            def _():
                self.main.wait_recv()

            self.relay()

            @pl.when(plane == self.last)
            def _():
                for _, _, _, final, leg in self.legs:
                    if final:
                        leg.wait_recv()

        def wait_send(self):
            @pl.when(plane != self.first)
            def _():
                self.main.wait_send()

            for source, _, _, _, leg in self.legs:

                @pl.when(plane == source)
                def _():
                    leg.wait_send()

    own = lambda s, j: obj.at[s] if j == 0 else reg.at[s, 0, j]
    z1_all = [Message("z1", s, obj.at[s], reg.at[s, 0, 1], relay_z.at[s, 0], GATHER_PARTS, -1) for s in range(2)]
    z2_all = [Message("z2", s, reg.at[s, 0, 1], reg.at[s, 0, 2], relay_z.at[s, 1], GATHER_PARTS, -1) for s in range(2)]
    z1 = lambda s: z1_all[s]
    z2 = lambda s: z2_all[s]
    step_a = lambda s, j: copy("a", s, j, own(s, j), reg.at[s, 1, j], at(-1, 0))
    step_b = lambda s, j: copy("b", s, j, own(s, j), reg.at[s, 2, j], at(-2, 0))
    step_f = lambda s, j: copy("f", s, j, reg.at[s, 1, j], reg.at[s, 2, j], at(-1, 0))
    full = lambda s: slice(0, 2 + s)
    q1 = lambda s, j: copy("q1", s, j, terms.at[s, 1, j, full(s)], rx_a.at[s, j, full(s)], at(1, 0))
    q1s = lambda s, j: copy("q1", s, j, tx.at[s, j, full(s)], rx_a.at[s, j, full(s)], at(1, 0))
    q2 = lambda s, j: copy("q2", s, j, terms.at[s, 2, j, full(s)], rx_b.at[s, j, full(s)], at(2, 0))
    q3 = lambda s, j: copy("q3", s, j, terms.at[s, 2, j, full(s)], rx_c.at[s, j, full(s)], at(1, 0))
    sums = lambda kind, s, k: Message(
        kind, s, tx.at[s, 3 + k, full(s)], rx_d.at[s, k, full(s)], relay_c.at[s, k, :, full(s)], SUM_PARTS, 1
    )
    c2_all = [sums("c2", s, 0) for s in range(2)]
    c1_all = [sums("c1", s, 1) for s in range(2)]
    c2 = lambda s: c2_all[s]
    c1 = lambda s: c1_all[s]
    near = [copy("o", 0, i - 1, places.at[0, 0], places.at[0, i], at(i, 0)) for i in (1, 2)]
    far = [copy("o", 0, j + 1, places.at[0], places.at[j], at(0, j)) for j in (1, 2)]

    def strip(s, j):
        step_a(s, j).start()

        @pl.when(odd)
        def _():
            step_b(s, j).start()

    for sent in near:
        sent.start()
    for s in range(2):
        z1(s).start()
        strip(s, 0)

    def mirrored(plain_re, plain_im, right, part):
        neg = -plain_im
        if right:
            part[0:width, 0:width] = plain_re
            part[0:width, width:] = plain_im
            part[width:, 0:width] = neg
            part[width:, width:] = plain_re
        else:
            part[0:width, 0:width] = plain_re
            part[0:width, width:] = neg
            part[width:, 0:width] = plain_im
            part[width:, width:] = plain_re

    for k in range(2):
        mirrored(atab[k], atab[2 + k], True, prop_r.at[k])
        mirrored(atab[k], atab[2 + k], False, prop_l.at[k])

    def one_hot(shift, axis):
        place = lax.broadcasted_iota(jnp.int32, (width, width), axis)
        other = lax.broadcasted_iota(jnp.int32, (width, width), 1 - axis)
        moved = place - shift
        moved = jnp.where(moved < 0, moved + width, moved)
        return jnp.where(moved == other, 1.0, 0.0).astype(BF16)

    rows_hot = one_hot(top, 0)
    cols_hot = one_hot(left, 1)
    for k in range(2):
        mirrored(dot(ftab[k], cols_hot).astype(BF16), dot(ftab[2 + k], cols_hot).astype(BF16), True, four_r.at[k])
        mirrored(dot(rows_hot, ftab[k]).astype(BF16), dot(rows_hot, ftab[2 + k]).astype(BF16), False, four_l.at[k])

    for k in range(2):
        total = None
        for part in split(probe[k]):
            moved = dot(dot(rows_hot, part).astype(BF16), cols_hot)
            total = moved if total is None else total + moved
        psi0[k] = total

    def put(k, rows, cols, value):
        high, low = split(value)
        base = k * width
        work[0, rows, base + cols.start : base + cols.stop] = high
        work[1, rows, base + cols.start : base + cols.stop] = low

    def sandwich(left_mat, right_mat):
        inner = dot(work[0], right_mat[0]) + (dot(work[1], right_mat[0]) + dot(work[0], right_mat[1]))
        for k in range(2):
            high, low = split(inner[:, k * width : (k + 1) * width])
            half[0, k * width : (k + 1) * width, :] = high
            half[1, k * width : (k + 1) * width, :] = low
        return dot(left_mat[0], half[0]) + (dot(left_mat[1], half[0]) + dot(left_mat[0], half[1]))

    everything = slice(0, width)
    for k in range(2):
        put(k, everything, everything, resid[k])
    both = sandwich(four_l, four_r)
    back1[0] = both[0:width]
    back1[1] = both[width:]

    rowm = lax.broadcasted_iota(jnp.int32, (tile, tile), 0) >= top
    colm = lax.broadcasted_iota(jnp.int32, (tile, tile), 1) >= left
    lo = slice(0, tile)
    hi = slice(tile, width)

    def piece(s, i, j, k):
        return obj[s, k] if i == 0 and j == 0 else reg[s, i, j, k]

    def quadrant(s, rows, cols, k):
        if rows is lo and cols is lo:
            return jnp.where(
                rowm,
                jnp.where(colm, piece(s, 0, 0, k), piece(s, 0, 2, k)),
                jnp.where(colm, piece(s, 2, 0, k), piece(s, 2, 2, k)),
            )
        if rows is lo:
            return jnp.where(rowm, piece(s, 0, 1, k), piece(s, 2, 1, k))
        if cols is lo:
            return jnp.where(colm, piece(s, 1, 0, k), piece(s, 1, 2, k))
        return piece(s, 1, 1, k)

    def scatter(s, ch, value):
        zero = jnp.zeros((tile, tile), F32)
        corner = value[lo, lo]
        upper = jnp.where(rowm, corner, zero)
        lower = jnp.where(rowm, zero, corner)
        terms[s, 0, 0, ch] = jnp.where(colm, upper, zero)
        terms[s, 0, 2, ch] = jnp.where(colm, zero, upper)
        terms[s, 2, 0, ch] = jnp.where(colm, lower, zero)
        terms[s, 2, 2, ch] = jnp.where(colm, zero, lower)
        corner = value[lo, hi]
        terms[s, 0, 1, ch] = jnp.where(rowm, corner, zero)
        terms[s, 2, 1, ch] = jnp.where(rowm, zero, corner)
        corner = value[hi, lo]
        terms[s, 1, 0, ch] = jnp.where(colm, corner, zero)
        terms[s, 1, 2, ch] = jnp.where(colm, zero, corner)
        terms[s, 1, 1, ch] = value[hi, hi]

    def arrivals(s):
        for j in range(3):
            step_a(s, j).wait_recv()

            @pl.when(odd)
            def _():
                step_f(s, j).start()

        for j in range(3):

            @pl.when(odd)
            def _():
                step_b(s, j).wait_recv()

            @pl.when(even)
            def _():
                step_f(s, j).wait_recv()

    for sent in near:
        sent.wait_recv()
    for sent in far:
        sent.start()
    for s in range(2):
        z1(s).wait_recv()
        z2(s).start()
        strip(s, 1)
    for s in range(2):
        z2(s).wait_recv()
        strip(s, 2)

    def send_terms(s):
        for j in (2, 1, 0):

            @pl.when(odd)
            def _():
                q2(s, j).start()

            @pl.when(even)
            def _():
                q3(s, j).start()
                q1(s, j).start()

    def send_sums(s):
        for j in (2, 1, 0):

            @pl.when(odd)
            def _():
                q3(s, j).wait_recv()
                tx[s, j, full(s)] = terms[s, 1, j, full(s)] + rx_c[s, j, full(s)]
                q1s(s, j).start()

    def row_total(s, j):
        q1(s, j).wait_recv()

        @pl.when(odd)
        def _():
            q2(s, j).wait_recv()

        @pl.when(odd)
        def _():
            terms[s, 0, j, full(s)] = terms[s, 0, j, full(s)] + (rx_a[s, j, full(s)] + rx_b[s, j, full(s)])

        @pl.when(even)
        def _():
            terms[s, 0, j, full(s)] = terms[s, 0, j, full(s)] + rx_a[s, j, full(s)]

        return terms[s, 0, j, full(s)]

    arrivals(0)
    for rows in (lo, hi):
        for cols in (lo, hi):
            obj_re, obj_im = quadrant(0, rows, cols, 0), quadrant(0, rows, cols, 1)
            psi_re, psi_im = psi0[0, rows, cols], psi0[1, rows, cols]
            put(0, rows, cols, psi_re * obj_re - psi_im * obj_im)
            put(1, rows, cols, psi_re * obj_im + psi_im * obj_re)
    both = sandwich(prop_l, prop_r)
    wave_re, wave_im = both[0:width], both[width:]
    scatter(1, 0, wave_re * back1[0] + wave_im * back1[1])
    scatter(1, 1, wave_re * back1[1] - wave_im * back1[0])
    scatter(1, 2, wave_re * wave_re + wave_im * wave_im)
    send_terms(1)

    send_sums(1)
    for sent in far:
        sent.wait_recv()
    light = split(probe[0] * probe[0] + probe[1] * probe[1])
    across = lax.broadcasted_iota(jnp.int32, (tile, tile), 1).astype(F32)
    down = lax.broadcasted_iota(jnp.int32, (tile, tile), 0).astype(F32)
    for i in range(3):
        for j in range(3):
            spot = (3 * j + i) * tile
            shift = places[j, i, 0:1, :]
            for k in range(2):
                hit = down + float(tile * (i - k)) - shift == across
                row_hot[spot : spot + tile, k * tile : (k + 1) * tile] = jnp.where(hit, 1.0, 0.0).astype(BF16)
            shift = places[j, i, 1:2, :]
            for k in range(2):
                hit = across + float(tile * (j - k)) - shift == down
                col_hot[3 * j + i, k * tile : (k + 1) * tile, :] = jnp.where(hit, 1.0, 0.0).astype(BF16)
    total = jnp.zeros((tile, tile), F32)
    for part in light:
        picked[...] = dot(row_hot[...], part).astype(BF16)
        for k in range(9):
            total = total + dot(picked[k * tile : (k + 1) * tile, :], col_hot[k])
    light0[...] = total

    tx[1, 3, full(1)] = row_total(1, 2)
    c2(1).start()
    middle = row_total(1, 1)
    c2(1).wait_recv()
    tx[1, 4, full(1)] = middle + rx_d[1, 0, full(1)]
    c1(1).start()
    arrivals(1)
    for rows in (lo, hi):
        for cols in (lo, hi):
            obj_re, obj_im = quadrant(1, rows, cols, 0), quadrant(1, rows, cols, 1)
            back_re, back_im = back1[0, rows, cols], back1[1, rows, cols]
            put(0, rows, cols, obj_re * back_re + obj_im * back_im)
            put(1, rows, cols, obj_im * back_re - obj_re * back_im)
    both = sandwich(prop_l, prop_r)
    conj_re, conj_im = both[0:width], both[width:]
    scatter(0, 0, psi0[0] * conj_re - psi0[1] * conj_im)
    scatter(0, 1, -(psi0[0] * conj_im + psi0[1] * conj_re))
    send_terms(0)

    send_sums(0)
    tx[0, 3, full(0)] = row_total(0, 2)
    c2(0).start()
    middle = row_total(0, 1)
    c2(0).wait_recv()
    tx[0, 4, full(0)] = middle + rx_d[0, 0, full(0)]
    c1(0).start()
    for s in (1, 0):
        last = row_total(s, 0)
        c1(s).wait_recv()
        total = last + rx_d[s, 1, full(s)]
        scale = STEP_SIZE / ((total[2] if s == 1 else light0[...]) + REGULAR)
        for k in range(2):
            out[s, k] = obj[s, k] - total[k] * scale

    for sent in near + far:
        sent.wait_send()
    for s in range(2):
        for sent in (z1(s), z2(s), c2(s), c1(s)):
            sent.wait_send()
        for j in range(3):
            step_a(s, j).wait_send()
            q1(s, j).wait_send()

            @pl.when(odd)
            def _():
                step_b(s, j).wait_send()
                step_f(s, j).wait_send()
                q2(s, j).wait_send()

            @pl.when(even)
            def _():
                q3(s, j).wait_send()


def solution(mesh):
    n_row, n_col = mesh.shape["row"], mesh.shape["col"]

    def local(object_slices, probe, offsets, residuals):
        layers, parts, tile, _ = object_slices.shape
        width = probe.shape[1]
        four, prop = tables(width)
        vmem = pl.BlockSpec(memory_space=pltpu.VMEM)
        stack = pltpu.VMEM((2, 2 * width, 2 * width), BF16)
        block = (3, tile, tile)
        call = pl.pallas_call(
            lambda *refs: kernel(n_row, n_col, *refs),
            out_shape=jax.ShapeDtypeStruct(object_slices.shape, F32),
            in_specs=[pl.BlockSpec(memory_space=pltpu.SMEM)] + [vmem] * 5,
            out_specs=vmem,
            scratch_shapes=[
                pltpu.VMEM((layers, 3, 3, parts, tile, tile), F32),
                pltpu.VMEM((2, width, 2 * width), BF16),
                stack, stack, stack, stack,
                pltpu.VMEM((2, 2 * width, width), BF16),
                pltpu.VMEM((2, width, width), F32),
                pltpu.VMEM((2, width, width), F32),
                pltpu.VMEM((layers, 3, 3) + block, F32),
                pltpu.VMEM((layers, 3) + block, F32),
                pltpu.VMEM((layers, 3) + block, F32),
                pltpu.VMEM((layers, 3) + block, F32),
                pltpu.VMEM((layers, 2) + block, F32),
                pltpu.VMEM((layers, 5) + block, F32),
                pltpu.VMEM((layers, 2, 2, parts, tile, tile), F32),
                pltpu.VMEM((layers, 2, 2) + block, F32),
                pltpu.VMEM((3, 3, 8, tile), F32),
                pltpu.VMEM((9 * tile, width), BF16),
                pltpu.VMEM((9, width, tile), BF16),
                pltpu.VMEM((9 * tile, width), BF16),
                pltpu.VMEM((tile, tile), F32),
                pltpu.SemaphoreType.DMA((len(SLOTS),)),
                pltpu.SemaphoreType.DMA((len(SLOTS),)),
            ],
            compiler_params=pltpu.CompilerParams(collective_id=0, has_side_effects=True, vmem_limit_bytes=56 * 1024 * 1024),
            name="ptycho",
        )
        return call(offsets.reshape(2), object_slices, probe, residuals[0, 0, 0], jnp.asarray(four), jnp.asarray(prop))

    placed = (
        P(None, None, "row", "col"),
        P(),
        P("row", "col", None, None),
        P("row", "col", None, None, None, None),
    )
    return jax.shard_map(local, mesh=mesh, in_specs=placed, out_specs=P(None, None, "row", "col"), check_vma=False)
```

```python
import math

import jax
import jax.numpy as jnp
import numpy as np
from jax import lax
from jax.experimental import pallas as pl
from jax.experimental.pallas import tpu as pltpu
from jax.sharding import PartitionSpec as P

FRESNEL = 40.0
STEP_SIZE = 0.5
REGULAR = 1.0
MESH = pl.DeviceIdType.MESH
F32 = jnp.float32
BF16 = jnp.bfloat16


def halves(mat):
    high = mat.astype(jnp.bfloat16)
    low = (mat - high.astype(np.float64)).astype(jnp.bfloat16)
    return [high, low]


def tables(width):
    index = np.arange(width)
    angle = 2.0 * math.pi / width * ((index[:, None] * index[None, :]) % width)
    inverse = np.exp(1j * angle) / math.sqrt(width)
    freq = np.where(index < width // 2, index, index - width) / width
    kern = np.exp(-1j * FRESNEL * math.pi * freq * freq)
    prop = (inverse * kern[None, :]) @ np.conj(inverse)
    pack = lambda mat: np.stack(halves(mat.real) + halves(mat.imag))
    return pack(inverse), pack(prop)


def split(value):
    high = value.astype(BF16)
    return high, (value - high.astype(F32)).astype(BF16)


def dot(left, right):
    return jnp.dot(left, right, preferred_element_type=F32)


GATHER_PARTS = (
    (0, 88, ((0, 0), (1, 7))),
    (88, 128, ((0, 0), (0, 7), (1, 7))),
)
SUM_PARTS = (
    ((0, 72, ((0, 7), (1, 0))), (72, 128, ((0, 7), (0, 0), (1, 0)))),
    ((0, 56, ((0, 7), (1, 0))), (56, 128, ((0, 7), (0, 0), (1, 0)))),
)
REROUTES = (((0, 1), (1, 0)), ((0, 2), (1, 1)), ((7, 0), (6, 1)))


def names():
    found = {}
    kinds = (("z1", 1), ("z2", 1), ("a", 3), ("b", 3), ("f", 3), ("q1", 3), ("q2", 3), ("q3", 3), ("c2", 1), ("c1", 1))
    for kind, count in kinds:
        for layer in range(2):
            for band in range(count):
                found[kind, layer, band] = len(found)
    for kind in ("z1", "z2", "c2", "c1"):
        for layer in range(2):
            for k, part in enumerate(GATHER_PARTS if kind[0] == "z" else SUM_PARTS[layer]):
                for leg in range(len(part[2]) - 1):
                    found[kind, layer, (k, leg)] = len(found)
    for kind in ("e", "g"):
        for layer in range(2):
            for k in range(len(REROUTES)):
                for i in (1, 2):
                    found[kind, layer, (i, k)] = len(found)
    for band in range(4):
        found["o", 0, band] = len(found)
    return found


SLOTS = names()


def kernel(
    n_row, n_col, offs, obj, probe, resid, ftab, atab, out,
    reg, work, four_r, four_l, prop_r, prop_l, half, psi0, back1, terms, rx_a, rx_b, rx_c, rx_d, rx_e, tx, relay_z, relay_c, places, row_hot, col_hot, picked, light0, ssem, rsem,
):
    tile = obj.shape[2]
    width = 2 * tile
    row = lax.axis_index("row")
    col = lax.axis_index("col")
    odd = lax.rem(row, 2) == 1
    even = lax.rem(row, 2) == 0
    at = lambda dr, dc: (lax.rem(row + dr + n_row, n_row), lax.rem(col + dc + n_col, n_col))

    depth = n_col // 2
    plane = lax.rem(col, depth)
    base = col - plane
    flipped = depth - base
    top = offs[0]
    left = offs[1]
    line = lax.broadcasted_iota(jnp.int32, places.shape[2:], 0)
    places[0, 0] = jnp.where(line == 0, top, left).astype(F32)

    barrier = pltpu.get_barrier_semaphore()
    greet = lambda who: pl.semaphore_signal(barrier, inc=1, device_id=who, device_id_type=MESH)
    for who in (at(0, -1), at(0, 1), at(0, -2), at(0, 2), at(-1, 0), at(1, 0), at(-2, 0), at(2, 0)):
        greet(who)
    count = 8
    hops = []
    for parts in (GATHER_PARTS, SUM_PARTS[0]):
        for _, _, path in parts:
            for leg in range(len(path) - 1):
                if len(path) > 2:
                    hops.append((path[leg], path[leg + 1]))

    def place_of(node, other):
        return (row, (base if node[0] == other[0] else flipped) + other[1])

    for first, second in hops:

        @pl.when(plane == first[1])
        def _():
            greet(place_of(first, second))

        @pl.when(plane == second[1])
        def _():
            greet(place_of(second, first))

        count = count + jnp.where(plane == first[1], 1, 0) + jnp.where(plane == second[1], 1, 0)
    pl.semaphore_wait(barrier, count)

    def copy(kind, layer, band, source, target, who):
        slot = SLOTS[kind, layer, band]
        return pltpu.make_async_remote_copy(
            src_ref=source, dst_ref=target, send_sem=ssem.at[slot], recv_sem=rsem.at[slot], device_id=who, device_id_type=MESH
        )

    class Message:
        def __init__(self, kind, layer, source, target, relay, parts, step):
            self.first, self.last = parts[0][2][0][1], parts[0][2][-1][1]
            self.main = copy(kind, layer, 0, source, target, at(0, step))
            self.legs = []
            for k, (low, high, path) in enumerate(parts):
                here = source.at[:, low:high]
                for leg in range(len(path) - 1):
                    final = leg == len(path) - 2
                    there = target.at[:, low:high] if final else relay.at[leg, :, low:high]
                    who = place_of(path[leg], path[leg + 1])
                    self.legs.append((path[leg][1], path[leg + 1][1], leg == 0, final, copy(kind, layer, (k, leg), here, there, who)))
                    here = there

        def start(self):
            @pl.when(plane != self.first)
            def _():
                self.main.start()

            @pl.when(plane == self.first)
            def _():
                for _, _, opening, _, leg in self.legs:
                    if opening:
                        leg.start()

        def relay(self):
            for k, (_, sink, _, final, leg) in enumerate(self.legs):
                if not final:
                    following = self.legs[k + 1][4]

                    @pl.when(plane == sink)
                    def _():
                        leg.wait_recv()
                        following.start()

        def wait_recv(self):
            @pl.when(plane != self.last)
            def _():
                self.main.wait_recv()

            self.relay()

            @pl.when(plane == self.last)
            def _():
                for _, _, _, final, leg in self.legs:
                    if final:
                        leg.wait_recv()

        def wait_send(self):
            @pl.when(plane != self.first)
            def _():
                self.main.wait_send()

            for source, _, _, _, leg in self.legs:

                @pl.when(plane == source)
                def _():
                    leg.wait_send()

    own = lambda s, j: obj.at[s] if j == 0 else reg.at[s, 0, j]
    z1_all = [Message("z1", s, obj.at[s], reg.at[s, 0, 1], relay_z.at[s, 0], GATHER_PARTS, -1) for s in range(2)]
    z2_all = [Message("z2", s, reg.at[s, 0, 1], reg.at[s, 0, 2], relay_z.at[s, 1], GATHER_PARTS, -1) for s in range(2)]
    z1 = lambda s: z1_all[s]
    z2 = lambda s: z2_all[s]
    step_a = lambda s, j: copy("a", s, j, own(s, j), reg.at[s, 1, j], at(-1, 0))
    step_b = lambda s, j: copy("b", s, j, own(s, j), reg.at[s, 2, j], at(-2, 0))
    step_f = lambda s, j: copy("f", s, j, reg.at[s, 1, j], reg.at[s, 2, j], at(-1, 0))
    full = lambda s: slice(0, 2 + s)
    q1 = lambda s, j: copy("q1", s, j, terms.at[s, 1, j, full(s)], rx_a.at[s, j, full(s)], at(1, 0))
    q1s = lambda s, j: copy("q1", s, j, tx.at[s, j, full(s)], rx_a.at[s, j, full(s)], at(1, 0))
    q2 = lambda s, j: copy("q2", s, j, terms.at[s, 2, j, full(s)], rx_b.at[s, j, full(s)], at(2, 0))
    q3 = lambda s, j: copy("q3", s, j, terms.at[s, 2, j, full(s)], rx_c.at[s, j, full(s)], at(1, 0))
    sums = lambda kind, s, k: Message(
        kind, s, tx.at[s, 3 + k, full(s)], rx_d.at[s, k, full(s)], relay_c.at[s, k, :, full(s)], SUM_PARTS[s], 1
    )
    c2_all = [sums("c2", s, 0) for s in range(2)]
    c1_all = [sums("c1", s, 1) for s in range(2)]
    c2 = lambda s: c2_all[s]
    c1 = lambda s: c1_all[s]
    near = [copy("o", 0, i - 1, places.at[0, 0], places.at[0, i], at(i, 0)) for i in (1, 2)]
    far = [copy("o", 0, j + 1, places.at[0], places.at[j], at(0, j)) for j in (1, 2)]

    def on(choices):
        found = plane < 0
        for choice in choices:
            found = found | (plane == choice)
        return found

    taken = [on([take[0] for take, _ in REROUTES if take[1] == j]) for j in range(3)]
    given = [on([give[0] for _, give in REROUTES if give[1] == j]) for j in range(3)]
    kept = [jnp.logical_not(which) for which in taken]
    takes = lambda j: [(k, odd & (plane == take[0])) for k, (take, _) in enumerate(REROUTES) if take[1] == j]
    gives = lambda j: [(k, odd & (plane == give[0])) for k, (_, give) in enumerate(REROUTES) if give[1] == j]

    def step_e(s, i, k):
        (to_plane, to_band), (from_plane, from_band) = REROUTES[k]
        return copy("e", s, (i, k), reg.at[s, i, from_band], reg.at[s, i, to_band], at(0, to_plane - from_plane))

    def step_g(s, i, k):
        (to_plane, to_band), (from_plane, _) = REROUTES[k]
        source = tx.at[s, to_band, full(s)] if i == 1 else terms.at[s, 2, to_band, full(s)]
        return copy("g", s, (i, k), source, rx_e.at[s, i - 1, k, full(s)], at(0, from_plane - to_plane))

    def when(condition, *acts):
        @pl.when(condition)
        def _():
            for act in acts:
                act()

    def strip(s, j):
        when(odd | kept[j], step_a(s, j).start)
        when(odd & kept[j], step_b(s, j).start)

    for sent in near:
        sent.start()
    for s in range(2):
        z1(s).start()
        strip(s, 0)

    def mirrored(plain_re, plain_im, right, part):
        neg = -plain_im
        if right:
            part[0:width, 0:width] = plain_re
            part[0:width, width:] = plain_im
            part[width:, 0:width] = neg
            part[width:, width:] = plain_re
        else:
            part[0:width, 0:width] = plain_re
            part[0:width, width:] = neg
            part[width:, 0:width] = plain_im
            part[width:, width:] = plain_re

    for k in range(2):
        mirrored(atab[k], atab[2 + k], True, prop_r.at[k])
        mirrored(atab[k], atab[2 + k], False, prop_l.at[k])

    def one_hot(shift, axis):
        place = lax.broadcasted_iota(jnp.int32, (width, width), axis)
        other = lax.broadcasted_iota(jnp.int32, (width, width), 1 - axis)
        moved = place - shift
        moved = jnp.where(moved < 0, moved + width, moved)
        return jnp.where(moved == other, 1.0, 0.0).astype(BF16)

    rows_hot = one_hot(top, 0)
    cols_hot = one_hot(left, 1)
    for k in range(2):
        mirrored(dot(ftab[k], cols_hot).astype(BF16), dot(ftab[2 + k], cols_hot).astype(BF16), True, four_r.at[k])
        mirrored(dot(rows_hot, ftab[k]).astype(BF16), dot(rows_hot, ftab[2 + k]).astype(BF16), False, four_l.at[k])

    for k in range(2):
        total = None
        for part in split(probe[k]):
            moved = dot(dot(rows_hot, part).astype(BF16), cols_hot)
            total = moved if total is None else total + moved
        psi0[k] = total

    def put(k, rows, cols, value):
        high, low = split(value)
        base = k * width
        work[0, rows, base + cols.start : base + cols.stop] = high
        work[1, rows, base + cols.start : base + cols.stop] = low

    def sandwich(left_mat, right_mat):
        inner = dot(work[0], right_mat[0]) + (dot(work[1], right_mat[0]) + dot(work[0], right_mat[1]))
        for k in range(2):
            high, low = split(inner[:, k * width : (k + 1) * width])
            half[0, k * width : (k + 1) * width, :] = high
            half[1, k * width : (k + 1) * width, :] = low
        return dot(left_mat[0], half[0]) + (dot(left_mat[1], half[0]) + dot(left_mat[0], half[1]))

    everything = slice(0, width)
    for k in range(2):
        put(k, everything, everything, resid[k])
    both = sandwich(four_l, four_r)
    back1[0] = both[0:width]
    back1[1] = both[width:]

    rowm = lax.broadcasted_iota(jnp.int32, (tile, tile), 0) >= top
    colm = lax.broadcasted_iota(jnp.int32, (tile, tile), 1) >= left
    lo = slice(0, tile)
    hi = slice(tile, width)

    def piece(s, i, j, k):
        return obj[s, k] if i == 0 and j == 0 else reg[s, i, j, k]

    def quadrant(s, rows, cols, k):
        if rows is lo and cols is lo:
            return jnp.where(
                rowm,
                jnp.where(colm, piece(s, 0, 0, k), piece(s, 0, 2, k)),
                jnp.where(colm, piece(s, 2, 0, k), piece(s, 2, 2, k)),
            )
        if rows is lo:
            return jnp.where(rowm, piece(s, 0, 1, k), piece(s, 2, 1, k))
        if cols is lo:
            return jnp.where(colm, piece(s, 1, 0, k), piece(s, 1, 2, k))
        return piece(s, 1, 1, k)

    def scatter(s, ch, value):
        zero = jnp.zeros((tile, tile), F32)
        corner = value[lo, lo]
        upper = jnp.where(rowm, corner, zero)
        lower = jnp.where(rowm, zero, corner)
        terms[s, 0, 0, ch] = jnp.where(colm, upper, zero)
        terms[s, 0, 2, ch] = jnp.where(colm, zero, upper)
        terms[s, 2, 0, ch] = jnp.where(colm, lower, zero)
        terms[s, 2, 2, ch] = jnp.where(colm, zero, lower)
        corner = value[lo, hi]
        terms[s, 0, 1, ch] = jnp.where(rowm, corner, zero)
        terms[s, 2, 1, ch] = jnp.where(rowm, zero, corner)
        corner = value[hi, lo]
        terms[s, 1, 0, ch] = jnp.where(colm, corner, zero)
        terms[s, 1, 2, ch] = jnp.where(colm, zero, corner)
        terms[s, 1, 1, ch] = value[hi, hi]

    def arrivals(s):
        for j in range(3):
            when(even | kept[j], step_a(s, j).wait_recv)
            for k, here in takes(j):
                when(here, step_e(s, 1, k).wait_recv)
            when(odd, step_f(s, j).start)
            for k, here in gives(j):
                when(here, step_e(s, 1, k).start)
            when(odd & kept[j], step_b(s, j).wait_recv)
            for k, here in takes(j):
                when(here, step_e(s, 2, k).wait_recv)
            for k, here in gives(j):
                when(here, step_e(s, 2, k).start)
        for j in range(3):
            when(even, step_f(s, j).wait_recv)

    for sent in near:
        sent.wait_recv()
    for sent in far:
        sent.start()
    for s in range(2):
        z1(s).wait_recv()
        z2(s).start()
        strip(s, 1)
    for s in range(2):
        z2(s).wait_recv()
        strip(s, 2)

    def send_terms(s):
        for j in (2, 1, 0):
            when(odd & kept[j] & jnp.logical_not(given[j]), q2(s, j).start)
            for k, here in takes(j):
                when(here, step_g(s, 2, k).start)
            when(even, q3(s, j).start, q1(s, j).start)

    def send_sums(s):
        for j in (2, 1, 0):

            @pl.when(odd)
            def _():
                q3(s, j).wait_recv()
                tx[s, j, full(s)] = terms[s, 1, j, full(s)] + rx_c[s, j, full(s)]

            for k, here in gives(j):

                @pl.when(here)
                def _():
                    step_g(s, 2, k).wait_recv()
                    terms[s, 2, j, full(s)] = terms[s, 2, j, full(s)] + rx_e[s, 1, k, full(s)]
                    q2(s, j).start()
                    step_g(s, 1, k).wait_recv()
                    tx[s, j, full(s)] = tx[s, j, full(s)] + rx_e[s, 0, k, full(s)]

            when(odd & kept[j], q1s(s, j).start)
            for k, here in takes(j):
                when(here, step_g(s, 1, k).start)

    def row_total(s, j):
        when(even & kept[j] | odd, q1(s, j).wait_recv)
        when(odd & kept[j], q2(s, j).wait_recv)

        def add(*others):
            total = terms[s, 0, j, full(s)]
            for other in others:
                total = total + other[s, j, full(s)]
            terms[s, 0, j, full(s)] = total

        when(odd & kept[j], lambda: add(rx_a, rx_b))
        when(even & kept[j] | odd & taken[j], lambda: add(rx_a))
        return terms[s, 0, j, full(s)]

    arrivals(0)
    for rows in (lo, hi):
        for cols in (lo, hi):
            obj_re, obj_im = quadrant(0, rows, cols, 0), quadrant(0, rows, cols, 1)
            psi_re, psi_im = psi0[0, rows, cols], psi0[1, rows, cols]
            put(0, rows, cols, psi_re * obj_re - psi_im * obj_im)
            put(1, rows, cols, psi_re * obj_im + psi_im * obj_re)
    both = sandwich(prop_l, prop_r)
    wave_re, wave_im = both[0:width], both[width:]
    scatter(1, 0, wave_re * back1[0] + wave_im * back1[1])
    scatter(1, 1, wave_re * back1[1] - wave_im * back1[0])
    scatter(1, 2, wave_re * wave_re + wave_im * wave_im)
    send_terms(1)

    def pass_columns(s):
        tx[s, 3, full(s)] = row_total(s, 2)
        c2(s).start()
        middle = row_total(s, 1)
        c2(s).wait_recv()
        tx[s, 4, full(s)] = middle + rx_d[s, 0, full(s)]
        c1(s).start()

    send_sums(1)
    for sent in far:
        sent.wait_recv()
    light = split(probe[0] * probe[0] + probe[1] * probe[1])
    across = lax.broadcasted_iota(jnp.int32, (tile, tile), 1).astype(F32)
    down = lax.broadcasted_iota(jnp.int32, (tile, tile), 0).astype(F32)
    for i in range(3):
        for j in range(3):
            spot = (3 * j + i) * tile
            shift = places[j, i, 0:1, :]
            for k in range(2):
                hit = down + float(tile * (i - k)) - shift == across
                row_hot[spot : spot + tile, k * tile : (k + 1) * tile] = jnp.where(hit, 1.0, 0.0).astype(BF16)
            shift = places[j, i, 1:2, :]
            for k in range(2):
                hit = across + float(tile * (j - k)) - shift == down
                col_hot[3 * j + i, k * tile : (k + 1) * tile, :] = jnp.where(hit, 1.0, 0.0).astype(BF16)
    total = jnp.zeros((tile, tile), F32)
    for part in light:
        picked[...] = dot(row_hot[...], part).astype(BF16)
        for k in range(9):
            total = total + dot(picked[k * tile : (k + 1) * tile, :], col_hot[k])
    light0[...] = total

    when(plane == depth - 1, lambda: pass_columns(1))

    arrivals(1)
    for rows in (lo, hi):
        for cols in (lo, hi):
            obj_re, obj_im = quadrant(1, rows, cols, 0), quadrant(1, rows, cols, 1)
            back_re, back_im = back1[0, rows, cols], back1[1, rows, cols]
            put(0, rows, cols, obj_re * back_re + obj_im * back_im)
            put(1, rows, cols, obj_im * back_re - obj_re * back_im)
    both = sandwich(prop_l, prop_r)
    conj_re, conj_im = both[0:width], both[width:]
    scatter(0, 0, psi0[0] * conj_re - psi0[1] * conj_im)
    scatter(0, 1, -(psi0[0] * conj_im + psi0[1] * conj_re))
    send_terms(0)

    when((plane != depth - 1) & (plane != 0), lambda: pass_columns(1))
    send_sums(0)
    when(plane == 0, lambda: pass_columns(1))
    pass_columns(0)
    for s in (1, 0):
        last = row_total(s, 0)
        c1(s).wait_recv()
        total = last + rx_d[s, 1, full(s)]
        scale = STEP_SIZE / ((total[2] if s == 1 else light0[...]) + REGULAR)
        for k in range(2):
            out[s, k] = obj[s, k] - total[k] * scale

    for sent in near + far:
        sent.wait_send()
    for s in range(2):
        for sent in (z1(s), z2(s), c2(s), c1(s)):
            sent.wait_send()
        for j in range(3):
            when(odd | kept[j], step_a(s, j).wait_send)
            when(even | kept[j], q1(s, j).wait_send)
            when(odd & kept[j], step_b(s, j).wait_send, q2(s, j).wait_send)
            when(odd, step_f(s, j).wait_send)
            when(even, q3(s, j).wait_send)
            for k, here in gives(j):
                when(here, step_e(s, 1, k).wait_send, step_e(s, 2, k).wait_send)
            for k, here in takes(j):
                when(here, step_g(s, 1, k).wait_send, step_g(s, 2, k).wait_send)


def solution(mesh):
    n_row, n_col = mesh.shape["row"], mesh.shape["col"]

    def local(object_slices, probe, offsets, residuals):
        layers, parts, tile, _ = object_slices.shape
        width = probe.shape[1]
        four, prop = tables(width)
        vmem = pl.BlockSpec(memory_space=pltpu.VMEM)
        stack = pltpu.VMEM((2, 2 * width, 2 * width), BF16)
        block = (3, tile, tile)
        call = pl.pallas_call(
            lambda *refs: kernel(n_row, n_col, *refs),
            out_shape=jax.ShapeDtypeStruct(object_slices.shape, F32),
            in_specs=[pl.BlockSpec(memory_space=pltpu.SMEM)] + [vmem] * 5,
            out_specs=vmem,
            scratch_shapes=[
                pltpu.VMEM((layers, 3, 3, parts, tile, tile), F32),
                pltpu.VMEM((2, width, 2 * width), BF16),
                stack, stack, stack, stack,
                pltpu.VMEM((2, 2 * width, width), BF16),
                pltpu.VMEM((2, width, width), F32),
                pltpu.VMEM((2, width, width), F32),
                pltpu.VMEM((layers, 3, 3) + block, F32),
                pltpu.VMEM((layers, 3) + block, F32),
                pltpu.VMEM((layers, 3) + block, F32),
                pltpu.VMEM((layers, 3) + block, F32),
                pltpu.VMEM((layers, 2) + block, F32),
                pltpu.VMEM((layers, 2, len(REROUTES)) + block, F32),
                pltpu.VMEM((layers, 5) + block, F32),
                pltpu.VMEM((layers, 2, 2, parts, tile, tile), F32),
                pltpu.VMEM((layers, 2, 2) + block, F32),
                pltpu.VMEM((3, 3, 8, tile), F32),
                pltpu.VMEM((9 * tile, width), BF16),
                pltpu.VMEM((9, width, tile), BF16),
                pltpu.VMEM((9 * tile, width), BF16),
                pltpu.VMEM((tile, tile), F32),
                pltpu.SemaphoreType.DMA((len(SLOTS),)),
                pltpu.SemaphoreType.DMA((len(SLOTS),)),
            ],
            compiler_params=pltpu.CompilerParams(collective_id=0, has_side_effects=True, vmem_limit_bytes=56 * 1024 * 1024),
            name="ptycho",
        )
        return call(offsets.reshape(2), object_slices, probe, residuals[0, 0, 0], jnp.asarray(four), jnp.asarray(prop))

    placed = (
        P(None, None, "row", "col"),
        P(),
        P("row", "col", None, None),
        P("row", "col", None, None, None, None),
    )
    return jax.shard_map(local, mesh=mesh, in_specs=placed, out_specs=P(None, None, "row", "col"), check_vma=False)
```

```python
import math

import jax
import jax.numpy as jnp
import numpy as np
from jax import lax
from jax.experimental import pallas as pl
from jax.experimental.pallas import tpu as pltpu
from jax.sharding import PartitionSpec as P

FRESNEL = 40.0
STEP_SIZE = 0.5
REGULAR = 1.0
MESH = pl.DeviceIdType.MESH
F32 = jnp.float32
BF16 = jnp.bfloat16


def halves(mat):
    high = mat.astype(jnp.bfloat16)
    low = (mat - high.astype(np.float64)).astype(jnp.bfloat16)
    return [high, low]


def tables(width):
    index = np.arange(width)
    angle = 2.0 * math.pi / width * ((index[:, None] * index[None, :]) % width)
    inverse = np.exp(1j * angle) / math.sqrt(width)
    freq = np.where(index < width // 2, index, index - width) / width
    kern = np.exp(-1j * FRESNEL * math.pi * freq * freq)
    prop = (inverse * kern[None, :]) @ np.conj(inverse)
    pack = lambda mat: np.stack(halves(mat.real) + halves(mat.imag))
    return pack(inverse), pack(prop)


def split(value):
    high = value.astype(BF16)
    return high, (value - high.astype(F32)).astype(BF16)


def dot(left, right):
    return jnp.dot(left, right, preferred_element_type=F32)


GATHER_PARTS = (
    (0, 88, ((0, 0), (1, 7))),
    (88, 128, ((0, 0), (0, 7), (1, 7))),
)
SUM_PARTS = (
    ((0, 80, ((0, 7), (1, 0))), (80, 128, ((0, 7), (0, 0), (1, 0)))),
    ((0, 72, ((0, 7), (1, 0))), (72, 128, ((0, 7), (0, 0), (1, 0)))),
)
REROUTES = (((0, 1), (1, 0)), ((0, 2), (1, 1)), ((7, 0), (6, 1)))


def names():
    found = {}
    kinds = (("z1", 1), ("z2", 1), ("a", 3), ("b", 3), ("f", 3), ("q1", 3), ("q2", 3), ("q3", 3), ("c2", 1), ("c1", 1))
    for kind, count in kinds:
        for layer in range(2):
            for band in range(count):
                found[kind, layer, band] = len(found)
    for kind in ("z1", "z2", "c2", "c1"):
        for layer in range(2):
            for k, part in enumerate(GATHER_PARTS if kind[0] == "z" else SUM_PARTS[layer]):
                for leg in range(len(part[2]) - 1):
                    found[kind, layer, (k, leg)] = len(found)
    for kind in ("e", "g"):
        for layer in range(2):
            for k in range(len(REROUTES)):
                for i in (1, 2):
                    found[kind, layer, (i, k)] = len(found)
    for band in range(4):
        found["o", 0, band] = len(found)
    return found


SLOTS = names()


def kernel(
    n_row, n_col, offs, obj, probe, resid, ftab, atab, out,
    reg, work, four_r, four_l, prop_r, prop_l, half, psi0, back1, terms, rx_a, rx_b, rx_c, rx_d, rx_e, tx, relay_z, relay_c, places, row_hot, col_hot, picked, light0, ssem, rsem,
):
    tile = obj.shape[2]
    width = 2 * tile
    row = lax.axis_index("row")
    col = lax.axis_index("col")
    odd = lax.rem(row, 2) == 1
    even = lax.rem(row, 2) == 0
    at = lambda dr, dc: (lax.rem(row + dr + n_row, n_row), lax.rem(col + dc + n_col, n_col))

    depth = n_col // 2
    plane = lax.rem(col, depth)
    base = col - plane
    flipped = depth - base
    top = offs[0]
    left = offs[1]
    line = lax.broadcasted_iota(jnp.int32, places.shape[2:], 0)
    places[0, 0] = jnp.where(line == 0, top, left).astype(F32)

    barrier = pltpu.get_barrier_semaphore()
    greet = lambda who: pl.semaphore_signal(barrier, inc=1, device_id=who, device_id_type=MESH)
    for who in (at(0, -1), at(0, 1), at(0, -2), at(0, 2), at(-1, 0), at(1, 0), at(-2, 0), at(2, 0)):
        greet(who)
    count = 8
    hops = []
    for parts in (GATHER_PARTS, SUM_PARTS[0]):
        for _, _, path in parts:
            for leg in range(len(path) - 1):
                if len(path) > 2:
                    hops.append((path[leg], path[leg + 1]))

    def place_of(node, other):
        return (row, (base if node[0] == other[0] else flipped) + other[1])

    for first, second in hops:

        @pl.when(plane == first[1])
        def _():
            greet(place_of(first, second))

        @pl.when(plane == second[1])
        def _():
            greet(place_of(second, first))

        count = count + jnp.where(plane == first[1], 1, 0) + jnp.where(plane == second[1], 1, 0)
    pl.semaphore_wait(barrier, count)

    def copy(kind, layer, band, source, target, who):
        slot = SLOTS[kind, layer, band]
        return pltpu.make_async_remote_copy(
            src_ref=source, dst_ref=target, send_sem=ssem.at[slot], recv_sem=rsem.at[slot], device_id=who, device_id_type=MESH
        )

    class Message:
        def __init__(self, kind, layer, source, target, relay, parts, step):
            self.first, self.last = parts[0][2][0][1], parts[0][2][-1][1]
            self.main = copy(kind, layer, 0, source, target, at(0, step))
            self.legs = []
            for k, (low, high, path) in enumerate(parts):
                here = source.at[:, low:high]
                for leg in range(len(path) - 1):
                    final = leg == len(path) - 2
                    there = target.at[:, low:high] if final else relay.at[leg, :, low:high]
                    who = place_of(path[leg], path[leg + 1])
                    self.legs.append((path[leg][1], path[leg + 1][1], leg == 0, final, copy(kind, layer, (k, leg), here, there, who)))
                    here = there

        def start(self):
            @pl.when(plane != self.first)
            def _():
                self.main.start()

            @pl.when(plane == self.first)
            def _():
                for _, _, opening, _, leg in self.legs:
                    if opening:
                        leg.start()

        def relay(self):
            for k, (_, sink, _, final, leg) in enumerate(self.legs):
                if not final:
                    following = self.legs[k + 1][4]

                    @pl.when(plane == sink)
                    def _():
                        leg.wait_recv()
                        following.start()

        def wait_recv(self):
            @pl.when(plane != self.last)
            def _():
                self.main.wait_recv()

            self.relay()

            @pl.when(plane == self.last)
            def _():
                for _, _, _, final, leg in self.legs:
                    if final:
                        leg.wait_recv()

        def wait_send(self):
            @pl.when(plane != self.first)
            def _():
                self.main.wait_send()

            for source, _, _, _, leg in self.legs:

                @pl.when(plane == source)
                def _():
                    leg.wait_send()

    own = lambda s, j: obj.at[s] if j == 0 else reg.at[s, 0, j]
    z1_all = [Message("z1", s, obj.at[s], reg.at[s, 0, 1], relay_z.at[s, 0], GATHER_PARTS, -1) for s in range(2)]
    z2_all = [Message("z2", s, reg.at[s, 0, 1], reg.at[s, 0, 2], relay_z.at[s, 1], GATHER_PARTS, -1) for s in range(2)]
    z1 = lambda s: z1_all[s]
    z2 = lambda s: z2_all[s]
    step_a = lambda s, j: copy("a", s, j, own(s, j), reg.at[s, 1, j], at(-1, 0))
    step_b = lambda s, j: copy("b", s, j, own(s, j), reg.at[s, 2, j], at(-2, 0))
    step_f = lambda s, j: copy("f", s, j, reg.at[s, 1, j], reg.at[s, 2, j], at(-1, 0))
    full = lambda s: slice(0, 2 + s)
    q1 = lambda s, j: copy("q1", s, j, terms.at[s, 1, j, full(s)], rx_a.at[s, j, full(s)], at(1, 0))
    q1s = lambda s, j: copy("q1", s, j, tx.at[s, j, full(s)], rx_a.at[s, j, full(s)], at(1, 0))
    q2 = lambda s, j: copy("q2", s, j, terms.at[s, 2, j, full(s)], rx_b.at[s, j, full(s)], at(2, 0))
    q3 = lambda s, j: copy("q3", s, j, terms.at[s, 2, j, full(s)], rx_c.at[s, j, full(s)], at(1, 0))
    sums = lambda kind, s, k: Message(
        kind, s, tx.at[s, 3 + k, full(s)], rx_d.at[s, k, full(s)], relay_c.at[s, k, :, full(s)], SUM_PARTS[s], 1
    )
    c2_all = [sums("c2", s, 0) for s in range(2)]
    c1_all = [sums("c1", s, 1) for s in range(2)]
    c2 = lambda s: c2_all[s]
    c1 = lambda s: c1_all[s]
    near = [copy("o", 0, i - 1, places.at[0, 0], places.at[0, i], at(i, 0)) for i in (1, 2)]
    far = [copy("o", 0, j + 1, places.at[0], places.at[j], at(0, j)) for j in (1, 2)]

    def on(choices):
        found = plane < 0
        for choice in choices:
            found = found | (plane == choice)
        return found

    taken = [on([take[0] for take, _ in REROUTES if take[1] == j]) for j in range(3)]
    given = [on([give[0] for _, give in REROUTES if give[1] == j]) for j in range(3)]
    kept = [jnp.logical_not(which) for which in taken]
    takes = lambda j: [(k, odd & (plane == take[0])) for k, (take, _) in enumerate(REROUTES) if take[1] == j]
    gives = lambda j: [(k, odd & (plane == give[0])) for k, (_, give) in enumerate(REROUTES) if give[1] == j]

    def step_e(s, i, k):
        (to_plane, to_band), (from_plane, from_band) = REROUTES[k]
        return copy("e", s, (i, k), reg.at[s, i, from_band], reg.at[s, i, to_band], at(0, to_plane - from_plane))

    def step_g(s, i, k):
        (to_plane, to_band), (from_plane, _) = REROUTES[k]
        source = tx.at[s, to_band, full(s)] if i == 1 else terms.at[s, 2, to_band, full(s)]
        return copy("g", s, (i, k), source, rx_e.at[s, i - 1, k, full(s)], at(0, from_plane - to_plane))

    def when(condition, *acts):
        @pl.when(condition)
        def _():
            for act in acts:
                act()

    def strip(s, j):
        when(odd | kept[j], step_a(s, j).start)
        when(odd & kept[j], step_b(s, j).start)

    for sent in near:
        sent.start()
    for s in range(2):
        z1(s).start()
        strip(s, 0)

    def mirrored(plain_re, plain_im, right, part):
        neg = -plain_im
        if right:
            part[0:width, 0:width] = plain_re
            part[0:width, width:] = plain_im
            part[width:, 0:width] = neg
            part[width:, width:] = plain_re
        else:
            part[0:width, 0:width] = plain_re
            part[0:width, width:] = neg
            part[width:, 0:width] = plain_im
            part[width:, width:] = plain_re

    for k in range(2):
        mirrored(atab[k], atab[2 + k], True, prop_r.at[k])
        mirrored(atab[k], atab[2 + k], False, prop_l.at[k])

    def one_hot(shift, axis):
        place = lax.broadcasted_iota(jnp.int32, (width, width), axis)
        other = lax.broadcasted_iota(jnp.int32, (width, width), 1 - axis)
        moved = place - shift
        moved = jnp.where(moved < 0, moved + width, moved)
        return jnp.where(moved == other, 1.0, 0.0).astype(BF16)

    rows_hot = one_hot(top, 0)
    cols_hot = one_hot(left, 1)
    for k in range(2):
        mirrored(dot(ftab[k], cols_hot).astype(BF16), dot(ftab[2 + k], cols_hot).astype(BF16), True, four_r.at[k])
        mirrored(dot(rows_hot, ftab[k]).astype(BF16), dot(rows_hot, ftab[2 + k]).astype(BF16), False, four_l.at[k])

    for k in range(2):
        total = None
        for part in split(probe[k]):
            moved = dot(dot(rows_hot, part).astype(BF16), cols_hot)
            total = moved if total is None else total + moved
        psi0[k] = total

    def put(k, rows, cols, value):
        high, low = split(value)
        base = k * width
        work[0, rows, base + cols.start : base + cols.stop] = high
        work[1, rows, base + cols.start : base + cols.stop] = low

    def sandwich(left_mat, right_mat):
        inner = dot(work[0], right_mat[0]) + (dot(work[1], right_mat[0]) + dot(work[0], right_mat[1]))
        for k in range(2):
            high, low = split(inner[:, k * width : (k + 1) * width])
            half[0, k * width : (k + 1) * width, :] = high
            half[1, k * width : (k + 1) * width, :] = low
        return dot(left_mat[0], half[0]) + (dot(left_mat[1], half[0]) + dot(left_mat[0], half[1]))

    everything = slice(0, width)
    for k in range(2):
        put(k, everything, everything, resid[k])
    both = sandwich(four_l, four_r)
    back1[0] = both[0:width]
    back1[1] = both[width:]

    rowm = lax.broadcasted_iota(jnp.int32, (tile, tile), 0) >= top
    colm = lax.broadcasted_iota(jnp.int32, (tile, tile), 1) >= left
    lo = slice(0, tile)
    hi = slice(tile, width)

    def piece(s, i, j, k):
        return obj[s, k] if i == 0 and j == 0 else reg[s, i, j, k]

    def quadrant(s, rows, cols, k):
        if rows is lo and cols is lo:
            return jnp.where(
                rowm,
                jnp.where(colm, piece(s, 0, 0, k), piece(s, 0, 2, k)),
                jnp.where(colm, piece(s, 2, 0, k), piece(s, 2, 2, k)),
            )
        if rows is lo:
            return jnp.where(rowm, piece(s, 0, 1, k), piece(s, 2, 1, k))
        if cols is lo:
            return jnp.where(colm, piece(s, 1, 0, k), piece(s, 1, 2, k))
        return piece(s, 1, 1, k)

    def scatter(s, ch, value):
        zero = jnp.zeros((tile, tile), F32)
        corner = value[lo, lo]
        upper = jnp.where(rowm, corner, zero)
        lower = jnp.where(rowm, zero, corner)
        terms[s, 0, 0, ch] = jnp.where(colm, upper, zero)
        terms[s, 0, 2, ch] = jnp.where(colm, zero, upper)
        terms[s, 2, 0, ch] = jnp.where(colm, lower, zero)
        terms[s, 2, 2, ch] = jnp.where(colm, zero, lower)
        corner = value[lo, hi]
        terms[s, 0, 1, ch] = jnp.where(rowm, corner, zero)
        terms[s, 2, 1, ch] = jnp.where(rowm, zero, corner)
        corner = value[hi, lo]
        terms[s, 1, 0, ch] = jnp.where(colm, corner, zero)
        terms[s, 1, 2, ch] = jnp.where(colm, zero, corner)
        terms[s, 1, 1, ch] = value[hi, hi]

    def arrivals(s):
        for j in range(3):
            when(even | kept[j], step_a(s, j).wait_recv)
            for k, here in takes(j):
                when(here, step_e(s, 1, k).wait_recv)
            when(odd, step_f(s, j).start)
            for k, here in gives(j):
                when(here, step_e(s, 1, k).start)
            when(odd & kept[j], step_b(s, j).wait_recv)
            for k, here in takes(j):
                when(here, step_e(s, 2, k).wait_recv)
            for k, here in gives(j):
                when(here, step_e(s, 2, k).start)
        for j in range(3):
            when(even, step_f(s, j).wait_recv)

    for sent in near:
        sent.wait_recv()
    for sent in far:
        sent.start()
    for s in range(2):
        z1(s).wait_recv()
        z2(s).start()
        strip(s, 1)
    for s in range(2):
        z2(s).wait_recv()
        strip(s, 2)

    def send_terms(s):
        for j in (2, 1, 0):
            when(odd & kept[j] & jnp.logical_not(given[j]), q2(s, j).start)
            for k, here in takes(j):
                when(here, step_g(s, 2, k).start)
            when(even, q3(s, j).start, q1(s, j).start)

    def send_sums(s):
        for j in (2, 1, 0):

            @pl.when(odd)
            def _():
                q3(s, j).wait_recv()
                tx[s, j, full(s)] = terms[s, 1, j, full(s)] + rx_c[s, j, full(s)]

            for k, here in gives(j):

                @pl.when(here)
                def _():
                    step_g(s, 2, k).wait_recv()
                    terms[s, 2, j, full(s)] = terms[s, 2, j, full(s)] + rx_e[s, 1, k, full(s)]
                    q2(s, j).start()
                    step_g(s, 1, k).wait_recv()
                    tx[s, j, full(s)] = tx[s, j, full(s)] + rx_e[s, 0, k, full(s)]

            when(odd & kept[j], q1s(s, j).start)
            for k, here in takes(j):
                when(here, step_g(s, 1, k).start)

    def row_total(s, j):
        when(even & kept[j] | odd, q1(s, j).wait_recv)
        when(odd & kept[j], q2(s, j).wait_recv)

        def add(*others):
            total = terms[s, 0, j, full(s)]
            for other in others:
                total = total + other[s, j, full(s)]
            terms[s, 0, j, full(s)] = total

        when(odd & kept[j], lambda: add(rx_a, rx_b))
        when(even & kept[j] | odd & taken[j], lambda: add(rx_a))
        return terms[s, 0, j, full(s)]

    arrivals(0)
    for rows in (lo, hi):
        for cols in (lo, hi):
            obj_re, obj_im = quadrant(0, rows, cols, 0), quadrant(0, rows, cols, 1)
            psi_re, psi_im = psi0[0, rows, cols], psi0[1, rows, cols]
            put(0, rows, cols, psi_re * obj_re - psi_im * obj_im)
            put(1, rows, cols, psi_re * obj_im + psi_im * obj_re)
    both = sandwich(prop_l, prop_r)
    wave_re, wave_im = both[0:width], both[width:]
    scatter(1, 0, wave_re * back1[0] + wave_im * back1[1])
    scatter(1, 1, wave_re * back1[1] - wave_im * back1[0])
    scatter(1, 2, wave_re * wave_re + wave_im * wave_im)
    send_terms(1)

    def open_columns(s):
        tx[s, 3, full(s)] = row_total(s, 2)
        c2(s).start()

    def close_columns(s):
        middle = row_total(s, 1)
        c2(s).wait_recv()
        tx[s, 4, full(s)] = middle + rx_d[s, 0, full(s)]
        c1(s).start()

    giver = on([give[0] for _, give in REROUTES])
    taker = on([take[0] for take, _ in REROUTES])
    middle_planes = jnp.logical_not(taker)
    when(giver, lambda: arrivals(1))
    send_sums(1)
    for sent in far:
        sent.wait_recv()
    light = split(probe[0] * probe[0] + probe[1] * probe[1])
    across = lax.broadcasted_iota(jnp.int32, (tile, tile), 1).astype(F32)
    down = lax.broadcasted_iota(jnp.int32, (tile, tile), 0).astype(F32)
    for i in range(3):
        for j in range(3):
            spot = (3 * j + i) * tile
            shift = places[j, i, 0:1, :]
            for k in range(2):
                hit = down + float(tile * (i - k)) - shift == across
                row_hot[spot : spot + tile, k * tile : (k + 1) * tile] = jnp.where(hit, 1.0, 0.0).astype(BF16)
            shift = places[j, i, 1:2, :]
            for k in range(2):
                hit = across + float(tile * (j - k)) - shift == down
                col_hot[3 * j + i, k * tile : (k + 1) * tile, :] = jnp.where(hit, 1.0, 0.0).astype(BF16)
    total = jnp.zeros((tile, tile), F32)
    for part in light:
        picked[...] = dot(row_hot[...], part).astype(BF16)
        for k in range(9):
            total = total + dot(picked[k * tile : (k + 1) * tile, :], col_hot[k])
    light0[...] = total

    when(taker, lambda: open_columns(1))
    when(plane == depth - 1, lambda: close_columns(1))

    when(jnp.logical_not(giver), lambda: arrivals(1))
    for rows in (lo, hi):
        for cols in (lo, hi):
            obj_re, obj_im = quadrant(1, rows, cols, 0), quadrant(1, rows, cols, 1)
            back_re, back_im = back1[0, rows, cols], back1[1, rows, cols]
            put(0, rows, cols, obj_re * back_re + obj_im * back_im)
            put(1, rows, cols, obj_im * back_re - obj_re * back_im)
    both = sandwich(prop_l, prop_r)
    conj_re, conj_im = both[0:width], both[width:]
    scatter(0, 0, psi0[0] * conj_re - psi0[1] * conj_im)
    scatter(0, 1, -(psi0[0] * conj_im + psi0[1] * conj_re))
    send_terms(0)

    when(middle_planes, lambda: open_columns(1))
    when(middle_planes, lambda: close_columns(1))
    send_sums(0)
    when(plane == 0, lambda: close_columns(1))
    open_columns(0)
    close_columns(0)
    for s in (1, 0):
        last = row_total(s, 0)
        c1(s).wait_recv()
        total = last + rx_d[s, 1, full(s)]
        scale = STEP_SIZE / ((total[2] if s == 1 else light0[...]) + REGULAR)
        for k in range(2):
            out[s, k] = obj[s, k] - total[k] * scale

    for sent in near + far:
        sent.wait_send()
    for s in range(2):
        for sent in (z1(s), z2(s), c2(s), c1(s)):
            sent.wait_send()
        for j in range(3):
            when(odd | kept[j], step_a(s, j).wait_send)
            when(even | kept[j], q1(s, j).wait_send)
            when(odd & kept[j], step_b(s, j).wait_send, q2(s, j).wait_send)
            when(odd, step_f(s, j).wait_send)
            when(even, q3(s, j).wait_send)
            for k, here in gives(j):
                when(here, step_e(s, 1, k).wait_send, step_e(s, 2, k).wait_send)
            for k, here in takes(j):
                when(here, step_g(s, 1, k).wait_send, step_g(s, 2, k).wait_send)


def solution(mesh):
    n_row, n_col = mesh.shape["row"], mesh.shape["col"]

    def local(object_slices, probe, offsets, residuals):
        layers, parts, tile, _ = object_slices.shape
        width = probe.shape[1]
        four, prop = tables(width)
        vmem = pl.BlockSpec(memory_space=pltpu.VMEM)
        stack = pltpu.VMEM((2, 2 * width, 2 * width), BF16)
        block = (3, tile, tile)
        call = pl.pallas_call(
            lambda *refs: kernel(n_row, n_col, *refs),
            out_shape=jax.ShapeDtypeStruct(object_slices.shape, F32),
            in_specs=[pl.BlockSpec(memory_space=pltpu.SMEM)] + [vmem] * 5,
            out_specs=vmem,
            scratch_shapes=[
                pltpu.VMEM((layers, 3, 3, parts, tile, tile), F32),
                pltpu.VMEM((2, width, 2 * width), BF16),
                stack, stack, stack, stack,
                pltpu.VMEM((2, 2 * width, width), BF16),
                pltpu.VMEM((2, width, width), F32),
                pltpu.VMEM((2, width, width), F32),
                pltpu.VMEM((layers, 3, 3) + block, F32),
                pltpu.VMEM((layers, 3) + block, F32),
                pltpu.VMEM((layers, 3) + block, F32),
                pltpu.VMEM((layers, 3) + block, F32),
                pltpu.VMEM((layers, 2) + block, F32),
                pltpu.VMEM((layers, 2, len(REROUTES)) + block, F32),
                pltpu.VMEM((layers, 5) + block, F32),
                pltpu.VMEM((layers, 2, 2, parts, tile, tile), F32),
                pltpu.VMEM((layers, 2, 2) + block, F32),
                pltpu.VMEM((3, 3, 8, tile), F32),
                pltpu.VMEM((9 * tile, width), BF16),
                pltpu.VMEM((9, width, tile), BF16),
                pltpu.VMEM((9 * tile, width), BF16),
                pltpu.VMEM((tile, tile), F32),
                pltpu.SemaphoreType.DMA((len(SLOTS),)),
                pltpu.SemaphoreType.DMA((len(SLOTS),)),
            ],
            compiler_params=pltpu.CompilerParams(collective_id=0, has_side_effects=True, vmem_limit_bytes=56 * 1024 * 1024),
            name="ptycho",
        )
        return call(offsets.reshape(2), object_slices, probe, residuals[0, 0, 0], jnp.asarray(four), jnp.asarray(prop))

    placed = (
        P(None, None, "row", "col"),
        P(),
        P("row", "col", None, None),
        P("row", "col", None, None, None, None),
    )
    return jax.shard_map(local, mesh=mesh, in_specs=placed, out_specs=P(None, None, "row", "col"), check_vma=False)
```

```python
import math

import jax
import jax.numpy as jnp
import numpy as np
from jax import lax
from jax.experimental import pallas as pl
from jax.experimental.pallas import tpu as pltpu
from jax.sharding import PartitionSpec as P

FRESNEL = 40.0
STEP_SIZE = 0.5
REGULAR = 1.0
MESH = pl.DeviceIdType.MESH
F32 = jnp.float32
BF16 = jnp.bfloat16


def halves(mat):
    high = mat.astype(jnp.bfloat16)
    low = (mat - high.astype(np.float64)).astype(jnp.bfloat16)
    return [high, low]


def tables(width):
    index = np.arange(width)
    angle = 2.0 * math.pi / width * ((index[:, None] * index[None, :]) % width)
    inverse = np.exp(1j * angle) / math.sqrt(width)
    freq = np.where(index < width // 2, index, index - width) / width
    kern = np.exp(-1j * FRESNEL * math.pi * freq * freq)
    prop = (inverse * kern[None, :]) @ np.conj(inverse)
    pack = lambda mat: np.stack(halves(mat.real) + halves(mat.imag))
    return pack(inverse), pack(prop)


def split(value):
    high = value.astype(BF16)
    return high, (value - high.astype(F32)).astype(BF16)


def dot(left, right):
    return jnp.dot(left, right, preferred_element_type=F32)


GATHER_PARTS = (
    (0, 96, ((0, 0), (1, 7))),
    (96, 128, ((0, 0), (0, 7), (1, 7))),
)
SUM_PARTS = (
    ((0, 80, ((0, 7), (1, 0))), (80, 128, ((0, 7), (0, 0), (1, 0)))),
    ((0, 72, ((0, 7), (1, 0))), (72, 128, ((0, 7), (0, 0), (1, 0)))),
)
REROUTES = (((0, 1), (1, 0)), ((0, 2), (1, 1)), ((7, 0), (6, 1)))


def names():
    found = {}
    kinds = (("z1", 1), ("z2", 1), ("a", 3), ("b", 3), ("f", 3), ("q1", 3), ("q2", 3), ("q3", 3), ("c2", 1), ("c1", 1))
    for kind, count in kinds:
        for layer in range(2):
            for band in range(count):
                found[kind, layer, band] = len(found)
    for kind in ("z1", "z2", "c2", "c1"):
        for layer in range(2):
            for k, part in enumerate(GATHER_PARTS if kind[0] == "z" else SUM_PARTS[layer]):
                for leg in range(len(part[2]) - 1):
                    found[kind, layer, (k, leg)] = len(found)
    for kind in ("e", "g"):
        for layer in range(2):
            for k in range(len(REROUTES)):
                for i in (1, 2):
                    found[kind, layer, (i, k)] = len(found)
    for band in range(4):
        found["o", 0, band] = len(found)
    return found


SLOTS = names()


def kernel(
    n_row, n_col, offs, obj, probe, resid, ftab, atab, out,
    reg, work, four_r, four_l, prop_r, prop_l, half, psi0, back1, terms, rx_a, rx_b, rx_c, rx_d, rx_e, tx, relay_z, relay_c, places, row_hot, col_hot, picked, light0, ssem, rsem,
):
    tile = obj.shape[2]
    width = 2 * tile
    row = lax.axis_index("row")
    col = lax.axis_index("col")
    odd = lax.rem(row, 2) == 1
    even = lax.rem(row, 2) == 0
    at = lambda dr, dc: (lax.rem(row + dr + n_row, n_row), lax.rem(col + dc + n_col, n_col))

    depth = n_col // 2
    plane = lax.rem(col, depth)
    base = col - plane
    flipped = depth - base
    top = offs[0]
    left = offs[1]
    line = lax.broadcasted_iota(jnp.int32, places.shape[2:], 0)
    places[0, 0] = jnp.where(line == 0, top, left).astype(F32)

    barrier = pltpu.get_barrier_semaphore()
    greet = lambda who: pl.semaphore_signal(barrier, inc=1, device_id=who, device_id_type=MESH)
    for who in (at(0, -1), at(0, 1), at(0, -2), at(0, 2), at(-1, 0), at(1, 0), at(-2, 0), at(2, 0)):
        greet(who)
    count = 8
    hops = []
    for parts in (GATHER_PARTS, SUM_PARTS[0]):
        for _, _, path in parts:
            for leg in range(len(path) - 1):
                if len(path) > 2:
                    hops.append((path[leg], path[leg + 1]))

    def place_of(node, other):
        return (row, (base if node[0] == other[0] else flipped) + other[1])

    for first, second in hops:

        @pl.when(plane == first[1])
        def _():
            greet(place_of(first, second))

        @pl.when(plane == second[1])
        def _():
            greet(place_of(second, first))

        count = count + jnp.where(plane == first[1], 1, 0) + jnp.where(plane == second[1], 1, 0)
    pl.semaphore_wait(barrier, count)

    def copy(kind, layer, band, source, target, who):
        slot = SLOTS[kind, layer, band]
        return pltpu.make_async_remote_copy(
            src_ref=source, dst_ref=target, send_sem=ssem.at[slot], recv_sem=rsem.at[slot], device_id=who, device_id_type=MESH
        )

    class Message:
        def __init__(self, kind, layer, source, target, relay, parts, step):
            self.first, self.last = parts[0][2][0][1], parts[0][2][-1][1]
            self.main = copy(kind, layer, 0, source, target, at(0, step))
            self.legs = []
            for k, (low, high, path) in enumerate(parts):
                here = source.at[:, low:high]
                for leg in range(len(path) - 1):
                    final = leg == len(path) - 2
                    there = target.at[:, low:high] if final else relay.at[leg, :, low:high]
                    who = place_of(path[leg], path[leg + 1])
                    self.legs.append((path[leg][1], path[leg + 1][1], leg == 0, final, copy(kind, layer, (k, leg), here, there, who)))
                    here = there

        def start(self):
            @pl.when(plane != self.first)
            def _():
                self.main.start()

            @pl.when(plane == self.first)
            def _():
                for _, _, opening, _, leg in self.legs:
                    if opening:
                        leg.start()

        def relay(self):
            for k, (_, sink, _, final, leg) in enumerate(self.legs):
                if not final:
                    following = self.legs[k + 1][4]

                    @pl.when(plane == sink)
                    def _():
                        leg.wait_recv()
                        following.start()

        def wait_recv(self):
            @pl.when(plane != self.last)
            def _():
                self.main.wait_recv()

            self.relay()

            @pl.when(plane == self.last)
            def _():
                for _, _, _, final, leg in self.legs:
                    if final:
                        leg.wait_recv()

        def wait_send(self):
            @pl.when(plane != self.first)
            def _():
                self.main.wait_send()

            for source, _, _, _, leg in self.legs:

                @pl.when(plane == source)
                def _():
                    leg.wait_send()

    own = lambda s, j: obj.at[s] if j == 0 else reg.at[s, 0, j]
    z1_all = [Message("z1", s, obj.at[s], reg.at[s, 0, 1], relay_z.at[s, 0], GATHER_PARTS, -1) for s in range(2)]
    z2_all = [Message("z2", s, reg.at[s, 0, 1], reg.at[s, 0, 2], relay_z.at[s, 1], GATHER_PARTS, -1) for s in range(2)]
    z1 = lambda s: z1_all[s]
    z2 = lambda s: z2_all[s]
    step_a = lambda s, j: copy("a", s, j, own(s, j), reg.at[s, 1, j], at(-1, 0))
    step_b = lambda s, j: copy("b", s, j, own(s, j), reg.at[s, 2, j], at(-2, 0))
    step_f = lambda s, j: copy("f", s, j, reg.at[s, 1, j], reg.at[s, 2, j], at(-1, 0))
    full = lambda s: slice(0, 2 + s)
    q1 = lambda s, j: copy("q1", s, j, terms.at[s, 1, j, full(s)], rx_a.at[s, j, full(s)], at(1, 0))
    q1s = lambda s, j: copy("q1", s, j, tx.at[s, j, full(s)], rx_a.at[s, j, full(s)], at(1, 0))
    q2 = lambda s, j: copy("q2", s, j, terms.at[s, 2, j, full(s)], rx_b.at[s, j, full(s)], at(2, 0))
    q3 = lambda s, j: copy("q3", s, j, terms.at[s, 2, j, full(s)], rx_c.at[s, j, full(s)], at(1, 0))
    sums = lambda kind, s, k: Message(
        kind, s, tx.at[s, 3 + k, full(s)], rx_d.at[s, k, full(s)], relay_c.at[s, k, :, full(s)], SUM_PARTS[s], 1
    )
    c2_all = [sums("c2", s, 0) for s in range(2)]
    c1_all = [sums("c1", s, 1) for s in range(2)]
    c2 = lambda s: c2_all[s]
    c1 = lambda s: c1_all[s]
    near = [copy("o", 0, i - 1, places.at[0, 0], places.at[0, i], at(i, 0)) for i in (1, 2)]
    far = [copy("o", 0, j + 1, places.at[0], places.at[j], at(0, j)) for j in (1, 2)]

    def on(choices):
        found = plane < 0
        for choice in choices:
            found = found | (plane == choice)
        return found

    taken = [on([take[0] for take, _ in REROUTES if take[1] == j]) for j in range(3)]
    given = [on([give[0] for _, give in REROUTES if give[1] == j]) for j in range(3)]
    kept = [jnp.logical_not(which) for which in taken]
    takes = lambda j: [(k, odd & (plane == take[0])) for k, (take, _) in enumerate(REROUTES) if take[1] == j]
    gives = lambda j: [(k, odd & (plane == give[0])) for k, (_, give) in enumerate(REROUTES) if give[1] == j]

    def step_e(s, i, k):
        (to_plane, to_band), (from_plane, from_band) = REROUTES[k]
        return copy("e", s, (i, k), reg.at[s, i, from_band], reg.at[s, i, to_band], at(0, to_plane - from_plane))

    def step_g(s, i, k):
        (to_plane, to_band), (from_plane, _) = REROUTES[k]
        source = tx.at[s, to_band, full(s)] if i == 1 else terms.at[s, 2, to_band, full(s)]
        return copy("g", s, (i, k), source, rx_e.at[s, i - 1, k, full(s)], at(0, from_plane - to_plane))

    def when(condition, *acts):
        @pl.when(condition)
        def _():
            for act in acts:
                act()

    def strip(s, j):
        when(odd | kept[j], step_a(s, j).start)
        when(odd & kept[j], step_b(s, j).start)

    for sent in near:
        sent.start()
    for s in range(2):
        z1(s).start()
        strip(s, 0)

    def mirrored(plain_re, plain_im, right, part):
        neg = -plain_im
        if right:
            part[0:width, 0:width] = plain_re
            part[0:width, width:] = plain_im
            part[width:, 0:width] = neg
            part[width:, width:] = plain_re
        else:
            part[0:width, 0:width] = plain_re
            part[0:width, width:] = neg
            part[width:, 0:width] = plain_im
            part[width:, width:] = plain_re

    for k in range(2):
        mirrored(atab[k], atab[2 + k], True, prop_r.at[k])
        mirrored(atab[k], atab[2 + k], False, prop_l.at[k])

    def one_hot(shift, axis):
        place = lax.broadcasted_iota(jnp.int32, (width, width), axis)
        other = lax.broadcasted_iota(jnp.int32, (width, width), 1 - axis)
        moved = place - shift
        moved = jnp.where(moved < 0, moved + width, moved)
        return jnp.where(moved == other, 1.0, 0.0).astype(BF16)

    rows_hot = one_hot(top, 0)
    cols_hot = one_hot(left, 1)
    for k in range(2):
        mirrored(dot(ftab[k], cols_hot).astype(BF16), dot(ftab[2 + k], cols_hot).astype(BF16), True, four_r.at[k])
        mirrored(dot(rows_hot, ftab[k]).astype(BF16), dot(rows_hot, ftab[2 + k]).astype(BF16), False, four_l.at[k])

    for k in range(2):
        total = None
        for part in split(probe[k]):
            moved = dot(dot(rows_hot, part).astype(BF16), cols_hot)
            total = moved if total is None else total + moved
        psi0[k] = total

    def put(k, rows, cols, value):
        high, low = split(value)
        base = k * width
        work[0, rows, base + cols.start : base + cols.stop] = high
        work[1, rows, base + cols.start : base + cols.stop] = low

    def sandwich(left_mat, right_mat):
        inner = dot(work[0], right_mat[0]) + (dot(work[1], right_mat[0]) + dot(work[0], right_mat[1]))
        for k in range(2):
            high, low = split(inner[:, k * width : (k + 1) * width])
            half[0, k * width : (k + 1) * width, :] = high
            half[1, k * width : (k + 1) * width, :] = low
        return dot(left_mat[0], half[0]) + (dot(left_mat[1], half[0]) + dot(left_mat[0], half[1]))

    everything = slice(0, width)
    for k in range(2):
        put(k, everything, everything, resid[k])
    both = sandwich(four_l, four_r)
    back1[0] = both[0:width]
    back1[1] = both[width:]

    rowm = lax.broadcasted_iota(jnp.int32, (tile, tile), 0) >= top
    colm = lax.broadcasted_iota(jnp.int32, (tile, tile), 1) >= left
    lo = slice(0, tile)
    hi = slice(tile, width)

    def piece(s, i, j, k):
        return obj[s, k] if i == 0 and j == 0 else reg[s, i, j, k]

    def quadrant(s, rows, cols, k):
        if rows is lo and cols is lo:
            return jnp.where(
                rowm,
                jnp.where(colm, piece(s, 0, 0, k), piece(s, 0, 2, k)),
                jnp.where(colm, piece(s, 2, 0, k), piece(s, 2, 2, k)),
            )
        if rows is lo:
            return jnp.where(rowm, piece(s, 0, 1, k), piece(s, 2, 1, k))
        if cols is lo:
            return jnp.where(colm, piece(s, 1, 0, k), piece(s, 1, 2, k))
        return piece(s, 1, 1, k)

    def scatter(s, ch, value):
        zero = jnp.zeros((tile, tile), F32)
        corner = value[lo, lo]
        upper = jnp.where(rowm, corner, zero)
        lower = jnp.where(rowm, zero, corner)
        terms[s, 0, 0, ch] = jnp.where(colm, upper, zero)
        terms[s, 0, 2, ch] = jnp.where(colm, zero, upper)
        terms[s, 2, 0, ch] = jnp.where(colm, lower, zero)
        terms[s, 2, 2, ch] = jnp.where(colm, zero, lower)
        corner = value[lo, hi]
        terms[s, 0, 1, ch] = jnp.where(rowm, corner, zero)
        terms[s, 2, 1, ch] = jnp.where(rowm, zero, corner)
        corner = value[hi, lo]
        terms[s, 1, 0, ch] = jnp.where(colm, corner, zero)
        terms[s, 1, 2, ch] = jnp.where(colm, zero, corner)
        terms[s, 1, 1, ch] = value[hi, hi]

    def arrivals(s):
        for j in range(3):
            when(even | kept[j], step_a(s, j).wait_recv)
            for k, here in takes(j):
                when(here, step_e(s, 1, k).wait_recv)
            when(odd, step_f(s, j).start)
            for k, here in gives(j):
                when(here, step_e(s, 1, k).start)
            when(odd & kept[j], step_b(s, j).wait_recv)
            for k, here in takes(j):
                when(here, step_e(s, 2, k).wait_recv)
            for k, here in gives(j):
                when(here, step_e(s, 2, k).start)
        for j in range(3):
            when(even, step_f(s, j).wait_recv)

    for sent in near:
        sent.wait_recv()
    for sent in far:
        sent.start()
    for s in range(2):
        z1(s).wait_recv()
        z2(s).start()
        strip(s, 1)
    for s in range(2):
        z2(s).wait_recv()
        strip(s, 2)

    def send_terms(s):
        for j in (2, 1, 0):
            when(odd & kept[j] & jnp.logical_not(given[j]), q2(s, j).start)
            for k, here in takes(j):
                when(here, step_g(s, 2, k).start)
            when(even, q3(s, j).start, q1(s, j).start)

    def send_sums(s):
        for j in (2, 1, 0):

            @pl.when(odd)
            def _():
                q3(s, j).wait_recv()
                tx[s, j, full(s)] = terms[s, 1, j, full(s)] + rx_c[s, j, full(s)]

            for k, here in gives(j):

                @pl.when(here)
                def _():
                    step_g(s, 2, k).wait_recv()
                    terms[s, 2, j, full(s)] = terms[s, 2, j, full(s)] + rx_e[s, 1, k, full(s)]
                    q2(s, j).start()
                    step_g(s, 1, k).wait_recv()
                    tx[s, j, full(s)] = tx[s, j, full(s)] + rx_e[s, 0, k, full(s)]

            when(odd & kept[j], q1s(s, j).start)
            for k, here in takes(j):
                when(here, step_g(s, 1, k).start)

    def row_total(s, j):
        when(even & kept[j] | odd, q1(s, j).wait_recv)
        when(odd & kept[j], q2(s, j).wait_recv)

        def add(*others):
            total = terms[s, 0, j, full(s)]
            for other in others:
                total = total + other[s, j, full(s)]
            terms[s, 0, j, full(s)] = total

        when(odd & kept[j], lambda: add(rx_a, rx_b))
        when(even & kept[j] | odd & taken[j], lambda: add(rx_a))
        return terms[s, 0, j, full(s)]

    arrivals(0)
    for rows in (lo, hi):
        for cols in (lo, hi):
            obj_re, obj_im = quadrant(0, rows, cols, 0), quadrant(0, rows, cols, 1)
            psi_re, psi_im = psi0[0, rows, cols], psi0[1, rows, cols]
            put(0, rows, cols, psi_re * obj_re - psi_im * obj_im)
            put(1, rows, cols, psi_re * obj_im + psi_im * obj_re)
    both = sandwich(prop_l, prop_r)
    wave_re, wave_im = both[0:width], both[width:]
    scatter(1, 0, wave_re * back1[0] + wave_im * back1[1])
    scatter(1, 1, wave_re * back1[1] - wave_im * back1[0])
    scatter(1, 2, wave_re * wave_re + wave_im * wave_im)
    send_terms(1)

    def open_columns(s):
        tx[s, 3, full(s)] = row_total(s, 2)
        c2(s).start()

    def close_columns(s):
        middle = row_total(s, 1)
        c2(s).wait_recv()
        tx[s, 4, full(s)] = middle + rx_d[s, 0, full(s)]
        c1(s).start()

    giver = on([give[0] for _, give in REROUTES])
    taker = on([take[0] for take, _ in REROUTES])
    middle_planes = jnp.logical_not(taker)
    when(giver, lambda: arrivals(1))
    send_sums(1)
    for sent in far:
        sent.wait_recv()
    light = split(probe[0] * probe[0] + probe[1] * probe[1])
    across = lax.broadcasted_iota(jnp.int32, (tile, tile), 1).astype(F32)
    down = lax.broadcasted_iota(jnp.int32, (tile, tile), 0).astype(F32)
    for i in range(3):
        for j in range(3):
            spot = (3 * j + i) * tile
            shift = places[j, i, 0:1, :]
            for k in range(2):
                hit = down + float(tile * (i - k)) - shift == across
                row_hot[spot : spot + tile, k * tile : (k + 1) * tile] = jnp.where(hit, 1.0, 0.0).astype(BF16)
            shift = places[j, i, 1:2, :]
            for k in range(2):
                hit = across + float(tile * (j - k)) - shift == down
                col_hot[3 * j + i, k * tile : (k + 1) * tile, :] = jnp.where(hit, 1.0, 0.0).astype(BF16)
    total = jnp.zeros((tile, tile), F32)
    for part in light:
        picked[...] = dot(row_hot[...], part).astype(BF16)
        for k in range(9):
            total = total + dot(picked[k * tile : (k + 1) * tile, :], col_hot[k])
    light0[...] = total

    when(taker, lambda: open_columns(1))
    when(plane == depth - 1, lambda: close_columns(1))

    when(jnp.logical_not(giver), lambda: arrivals(1))
    for rows in (lo, hi):
        for cols in (lo, hi):
            obj_re, obj_im = quadrant(1, rows, cols, 0), quadrant(1, rows, cols, 1)
            back_re, back_im = back1[0, rows, cols], back1[1, rows, cols]
            put(0, rows, cols, obj_re * back_re + obj_im * back_im)
            put(1, rows, cols, obj_im * back_re - obj_re * back_im)
    both = sandwich(prop_l, prop_r)
    conj_re, conj_im = both[0:width], both[width:]
    scatter(0, 0, psi0[0] * conj_re - psi0[1] * conj_im)
    scatter(0, 1, -(psi0[0] * conj_im + psi0[1] * conj_re))
    send_terms(0)

    when(middle_planes, lambda: open_columns(1))
    when(middle_planes, lambda: close_columns(1))
    send_sums(0)
    when(plane == 0, lambda: close_columns(1))
    open_columns(0)
    close_columns(0)
    for s in (1, 0):
        last = row_total(s, 0)
        c1(s).wait_recv()
        total = last + rx_d[s, 1, full(s)]
        scale = STEP_SIZE / ((total[2] if s == 1 else light0[...]) + REGULAR)
        for k in range(2):
            out[s, k] = obj[s, k] - total[k] * scale

    for sent in near + far:
        sent.wait_send()
    for s in range(2):
        for sent in (z1(s), z2(s), c2(s), c1(s)):
            sent.wait_send()
        for j in range(3):
            when(odd | kept[j], step_a(s, j).wait_send)
            when(even | kept[j], q1(s, j).wait_send)
            when(odd & kept[j], step_b(s, j).wait_send, q2(s, j).wait_send)
            when(odd, step_f(s, j).wait_send)
            when(even, q3(s, j).wait_send)
            for k, here in gives(j):
                when(here, step_e(s, 1, k).wait_send, step_e(s, 2, k).wait_send)
            for k, here in takes(j):
                when(here, step_g(s, 1, k).wait_send, step_g(s, 2, k).wait_send)


def solution(mesh):
    n_row, n_col = mesh.shape["row"], mesh.shape["col"]

    def local(object_slices, probe, offsets, residuals):
        layers, parts, tile, _ = object_slices.shape
        width = probe.shape[1]
        four, prop = tables(width)
        vmem = pl.BlockSpec(memory_space=pltpu.VMEM)
        stack = pltpu.VMEM((2, 2 * width, 2 * width), BF16)
        block = (3, tile, tile)
        call = pl.pallas_call(
            lambda *refs: kernel(n_row, n_col, *refs),
            out_shape=jax.ShapeDtypeStruct(object_slices.shape, F32),
            in_specs=[pl.BlockSpec(memory_space=pltpu.SMEM)] + [vmem] * 5,
            out_specs=vmem,
            scratch_shapes=[
                pltpu.VMEM((layers, 3, 3, parts, tile, tile), F32),
                pltpu.VMEM((2, width, 2 * width), BF16),
                stack, stack, stack, stack,
                pltpu.VMEM((2, 2 * width, width), BF16),
                pltpu.VMEM((2, width, width), F32),
                pltpu.VMEM((2, width, width), F32),
                pltpu.VMEM((layers, 3, 3) + block, F32),
                pltpu.VMEM((layers, 3) + block, F32),
                pltpu.VMEM((layers, 3) + block, F32),
                pltpu.VMEM((layers, 3) + block, F32),
                pltpu.VMEM((layers, 2) + block, F32),
                pltpu.VMEM((layers, 2, len(REROUTES)) + block, F32),
                pltpu.VMEM((layers, 5) + block, F32),
                pltpu.VMEM((layers, 2, 2, parts, tile, tile), F32),
                pltpu.VMEM((layers, 2, 2) + block, F32),
                pltpu.VMEM((3, 3, 8, tile), F32),
                pltpu.VMEM((9 * tile, width), BF16),
                pltpu.VMEM((9, width, tile), BF16),
                pltpu.VMEM((9 * tile, width), BF16),
                pltpu.VMEM((tile, tile), F32),
                pltpu.SemaphoreType.DMA((len(SLOTS),)),
                pltpu.SemaphoreType.DMA((len(SLOTS),)),
            ],
            compiler_params=pltpu.CompilerParams(collective_id=0, has_side_effects=True, vmem_limit_bytes=56 * 1024 * 1024),
            name="ptycho",
        )
        return call(offsets.reshape(2), object_slices, probe, residuals[0, 0, 0], jnp.asarray(four), jnp.asarray(prop))

    placed = (
        P(None, None, "row", "col"),
        P(),
        P("row", "col", None, None),
        P("row", "col", None, None, None, None),
    )
    return jax.shard_map(local, mesh=mesh, in_specs=placed, out_specs=P(None, None, "row", "col"), check_vma=False)
```
